16 devices in a mesh: dp: 4 (over y, z, core), sp: 4 (over x).
Axes of the slice: x: 4, y: 2, z: 1, core: 2. Of those that a mesh axis runs over, the one named last changes fastest.
The devices are a block of a 4x4x8 slice.
Arguments:
- x: bfloat16 [16384, 2048], P(('dp', 'sp')), parts along dimension 0
- gain: bfloat16 [2048], replicated
- wq: bfloat16 [2048, 4096], P('sp')
- wk: bfloat16 [2048, 2048], P('sp')
- wv: bfloat16 [2048, 2048], P('sp')
- wo: bfloat16 [4096, 2048], P('sp')
Outputs:
- output: bfloat16 [16384, 2048], P(('dp', 'sp')), parts along dimension 0
There are 4 independent parts. The reference program is written for one: setup_inputs(seed, part) draws one part's arguments, and reference() takes and returns one part's arrays. A program takes and returns all parts, laid end to end along the dimension named above; an argument that names none is the same for every part.
All inputs are finite; a program needn't handle non-finite values.
Results may differ from the reference program's by a relative error of at most 0.012.
Values are sent between devices in bfloat16 or wider.
A program may use at most 768 MiB of HBM per device.

```python
import jax
import jax.numpy as jnp
from jax import lax

ROWS = 4096
D = 2048
HEADS = 32
KV_HEADS = 16
HEAD = 128
THETA = 10000


def setup_inputs(seed: int = 0, part: int = 0) -> dict:
    kx, kn, kq, kk, kv, ko = jax.random.split(jax.random.key(seed), 6)

    def weights(key, rows, columns):
        return jax.random.normal(key, (rows, columns), jnp.float32) * rows**-0.5

    drawn = {
        "x": jax.random.normal(jax.random.fold_in(kx, part), (ROWS, D), jnp.float32),
        "gain": 1 + 0.1 * jax.random.normal(kn, (D,), jnp.float32),
        "wq": 2 * weights(kq, D, HEADS * HEAD),
        "wk": 2 * weights(kk, D, KV_HEADS * HEAD),
        "wv": 4 * weights(kv, D, KV_HEADS * HEAD),
        "wo": weights(ko, HEADS * HEAD, D),
    }
    return {k: v.astype(jnp.bfloat16) for k, v in drawn.items()}


def normed(x, gain):
    wide = x.astype(jnp.float32)
    scale = lax.rsqrt(jnp.mean(wide * wide, -1, keepdims=True) + 1e-6)
    return (wide * scale * gain.astype(jnp.float32)).astype(jnp.bfloat16)


def turned(t, place, theta):
    half = t.shape[-1] // 2
    angle = place.astype(jnp.float32)[:, None] * theta ** (-jnp.arange(half, dtype=jnp.float32) / half)
    cos, sin = jnp.cos(angle)[:, None], jnp.sin(angle)[:, None]
    a, b = t[..., :half].astype(jnp.float32), t[..., half:].astype(jnp.float32)
    return jnp.concatenate([a * cos - b * sin, b * cos + a * sin], -1).astype(jnp.bfloat16)


def matmul(a, w):
    return jnp.dot(a, w, preferred_element_type=jnp.float32).astype(jnp.bfloat16)


def einsum(form, a, b):
    return jnp.einsum(form, a.astype(jnp.float32), b.astype(jnp.float32))


def attention(q, k, v):
    scores = einsum("tgsd,ugd->gstu", q, k) * q.shape[-1] ** -0.5
    token = jnp.arange(q.shape[0])
    scores = jnp.where(token[:, None] >= token, scores, -jnp.inf)
    weights = jax.nn.softmax(scores, -1).astype(jnp.bfloat16)
    return einsum("gstu,ugd->tgsd", weights, v).astype(jnp.bfloat16)


def reference(x, gain, wq, wk, wv, wo):
    a, place = normed(x, gain), jnp.arange(ROWS)
    q = turned(matmul(a, wq).reshape(ROWS, HEADS, HEAD), place, THETA).reshape(ROWS, KV_HEADS, -1, HEAD)
    k = turned(matmul(a, wk).reshape(ROWS, KV_HEADS, HEAD), place, THETA)
    v = matmul(a, wv).reshape(ROWS, KV_HEADS, HEAD)
    seen = attention(q, k, v).reshape(ROWS, HEADS * HEAD)
    return (x.astype(jnp.float32) + jnp.dot(seen, wo, preferred_element_type=jnp.float32)).astype(jnp.bfloat16)
```

```python
import functools

import jax
import jax.numpy as jnp
from jax import lax
from jax.experimental import pallas as pl
from jax.experimental.pallas import tpu as pltpu
from jax.sharding import PartitionSpec as P

HEAD = 128
THETA = 10000
NEG = -1e30
HIDDEN = 2 * NEG
LOG2E = 1.4426950408889634
VMEM = 56 * 2**20
ANY = pl.BlockSpec(memory_space=pl.ANY)


def normed(x, gain):
    wide = x.astype(jnp.float32)
    scale = lax.rsqrt(jnp.mean(wide * wide, -1, keepdims=True) + 1e-6)
    return (wide * scale * gain.astype(jnp.float32)).astype(jnp.bfloat16)


def turns(tokens, theta):
    half = HEAD // 2
    angle = jnp.arange(tokens).astype(jnp.float32)[:, None] * theta ** (-jnp.arange(half, dtype=jnp.float32) / half)
    cos, sin = jnp.cos(angle), jnp.sin(angle)
    return jnp.concatenate([cos, cos], 1), jnp.concatenate([-sin, sin], 1)


def _dot(a, b, ca, cb):
    return lax.dot_general(a, b, (((ca,), (cb,)), ((), ())), preferred_element_type=jnp.float32)


def _project(at_ref, a0, a1, cos_ref, sin_ref, wq, wk, wv, near, far, near2, far2, *rest, alias, wide):
    q_out, k_out, v_out, w, sem = rest[3:] if alias else rest
    step = pl.program_id(0)
    depth = w.shape[0] // 4
    part = depth // 4
    nq, nk = q_out.shape[0] * HEAD, k_out.shape[0] * HEAD

    @pl.when(step == 0)
    def _():
        me, quad = at_ref[2], at_ref[3]
        own = pl.ds(me * depth, depth)
        copies = [
            pltpu.make_async_copy(wq.at[:, pl.ds(me * nq, nq)], w.at[own, pl.ds(0, nq)], sem),
            pltpu.make_async_copy(wk.at[:, pl.ds(me * nk, nk)], w.at[own, pl.ds(nq, nk)], sem),
            pltpu.make_async_copy(wv.at[:, pl.ds(me * nk, nk)], w.at[own, pl.ds(nq + nk, nk)], sem),
        ]
        for place, held in ((0, near), (2, far), (1, near2), (3, far2)):
            for i, shift in enumerate((3, 1, 2)):
                at = lax.rem(me + shift, 4) * depth + jnp.bitwise_xor(quad, place) * part
                copies.append(pltpu.make_async_copy(held.at[i], w.at[pl.ds(at, part), :], sem))
        for c in copies:
            c.start()
        for c in copies:
            c.wait()

    def run(a_ref):
        for at in range(0, w.shape[1], wide):
            got = jnp.dot(a_ref[...], w[:, at : at + wide], preferred_element_type=jnp.float32).astype(jnp.bfloat16)
            for h in range(at, at + wide, HEAD):
                t = got[:, h - at : h - at + HEAD]
                if h < nq + nk:
                    t = t.astype(jnp.float32)
                    t = (t * cos_ref[...] + pltpu.roll(t, HEAD // 2, 1) * sin_ref[...]).astype(jnp.bfloat16)
                if h < nq:
                    q_out[h // HEAD] = t
                elif h < nq + nk:
                    k_out[(h - nq) // HEAD] = t
                else:
                    v_out[(h - nq - nk) // HEAD] = t

    pl.when(step == 0)(lambda: run(a0))
    pl.when(step == 1)(lambda: run(a1))


def project(at, a0, a1, cos, sin, weights, held, before):
    wq, wk, wv = weights
    run, d = a0.shape
    tokens = cos.shape[0]
    qh, kh = wq.shape[1] // (4 * HEAD), wk.shape[1] // (4 * HEAD)
    cols = (qh + 2 * kh) * HEAD
    whole = pl.BlockSpec((run, d), lambda i, at: (0, 0))
    table = pl.BlockSpec((run, HEAD), lambda i, at: (at[i], 0))
    outs = [pl.BlockSpec((h, run, HEAD), lambda i, at: (0, at[i], 0)) for h in (qh, kh, kh)]
    given = [a0, a1, cos, sin, wq, wk, wv, *held] + list(before or ())
    return pl.pallas_call(
        functools.partial(_project, alias=before is not None, wide=512),
        grid_spec=pltpu.PrefetchScalarGridSpec(
            num_scalar_prefetch=1,
            grid=(2,),
            in_specs=[whole, whole, table, table] + [ANY] * (len(given) - 4),
            out_specs=outs,
            scratch_shapes=[pltpu.VMEM((d, cols), jnp.bfloat16), pltpu.SemaphoreType.DMA],
        ),
        out_shape=[jax.ShapeDtypeStruct((h, tokens, HEAD), jnp.bfloat16) for h in (qh, kh, kh)],
        input_output_aliases={12: 0, 13: 1, 14: 2} if before is not None else {},
        compiler_params=pltpu.CompilerParams(dimension_semantics=("arbitrary",), vmem_limit_bytes=VMEM),
        cost_estimate=pl.CostEstimate(flops=4 * run * d * cols, transcendentals=0, bytes_accessed=2 * (d * cols + 2 * run * (d + cols))),
        name="project",
    )(at, *given)


def _attend(q_ref, k_ref, v_ref, o_ref, top_s, mix_s, *, scale, bq, bk, wide):
    kb, d = k_ref.shape[0], k_ref.shape[2]
    g = q_ref.shape[0] // kb
    cols = g * bq
    iq = pl.program_id(0)
    e = scale * LOG2E
    pieces = [(i, at) for i in range(kb) for at in range(0, cols, wide)]
    top_s[...] = jnp.full(top_s.shape, NEG, jnp.float32)
    mix_s[...] = jnp.zeros(mix_s.shape, jnp.float32)
    ones = jnp.ones((8, bk), k_ref.dtype)

    def block(j, masked):
        here = pl.ds(pl.multiple_of(j * bk, bk), bk)
        scores = [_dot(k_ref[i, here, :], q_ref[g * i : g * i + g].reshape(cols, d)[at : at + wide, :], 1, 1) for i, at in pieces]
        weights, keeps = [], []
        for (i, at), s in zip(pieces, scores):
            if masked:
                gap = lax.rem(lax.broadcasted_iota(jnp.int32, (bk, wide), 1) + at, bq) - lax.broadcasted_iota(jnp.int32, (bk, wide), 0)
                s = jnp.where(gap >= j * bk - iq * bq, s, HIDDEN)
            old = top_s[i : i + 1, at : at + wide]
            top = jnp.maximum(old, s.max(axis=0, keepdims=True))
            top_s[i : i + 1, at : at + wide] = top
            weights.append(jnp.exp2((s - top) * e).astype(k_ref.dtype))
            keeps.append(jnp.exp2((old - top) * e))
        for (i, at), p, keep in zip(pieces, weights, keeps):
            values = jnp.concatenate([v_ref[i, here, :].T, ones], axis=0)
            mix_s[i, :, at : at + wide] = mix_s[i, :, at : at + wide] * keep + _dot(values, p, 1, 0)

    whole = iq * bq // bk
    lax.fori_loop(0, whole, lambda j, _: block(j, False), None)
    for n in range(max(bq // bk, 1)):
        block(whole + n, True)

    for i in range(kb):
        o = (mix_s[i, :d, :] * (1 / mix_s[i, d : d + 1, :])).T.astype(o_ref.dtype)
        for n in range(g):
            o_ref[:, (g * i + n) * d : (g * i + n + 1) * d] = o[n * bq : (n + 1) * bq]


def attend(q, k, v, first, kb, bq=512, bk=512, wide=512):
    h, tokens, d = q.shape
    g = h // k.shape[0]
    keys = pl.BlockSpec((kb, tokens, d), lambda i: (first, 0, 0))
    return pl.pallas_call(
        functools.partial(_attend, scale=d**-0.5, bq=bq, bk=bk, wide=wide),
        grid=(tokens // bq,),
        in_specs=[pl.BlockSpec((kb * g, bq, d), lambda i: (first, i, 0)), keys, keys],
        out_specs=pl.BlockSpec((bq, kb * g * d), lambda i: (i, 0)),
        out_shape=jax.ShapeDtypeStruct((tokens, kb * g * d), q.dtype),
        scratch_shapes=[pltpu.VMEM((kb, g * bq), jnp.float32), pltpu.VMEM((kb, d + 8, g * bq), jnp.float32)],
        compiler_params=pltpu.CompilerParams(dimension_semantics=("arbitrary",), vmem_limit_bytes=VMEM),
        cost_estimate=pl.CostEstimate(flops=4 * kb * g * tokens * tokens * d, transcendentals=kb * g * tokens * tokens // 2,
                                      bytes_accessed=2 * kb * tokens * d * (2 + 2 * g)),
        name="attend",
    )(q, k, v)


def _output(at_ref, s0, s1, s2, s3, before, wo, near, far, near2, far2, o_ref, w, sem, *, quarters):
    step = pl.program_id(0)
    depth = near.shape[1]

    @pl.when(step == 0)
    def _():
        quad = at_ref[1]
        copies = []
        for n, quarter in enumerate(quarters):
            copies.append(pltpu.make_async_copy(wo.at[pl.ds(quarter * depth, depth)], w.at[0, pl.ds(n * depth, depth)], sem))
            copies[-1].start()
            for i in range(3):
                put = w.at[1 + i, pl.ds(n * depth, depth)]
                for place, held in ((0, near), (2, far), (1, near2), (3, far2)):

                    @pl.when(jnp.bitwise_xor(quad, place) == quarter)
                    def _():
                        pltpu.make_async_copy(held.at[i], put, sem).start()

                copies.append(pltpu.make_async_copy(near.at[i], put, sem))
        for c in copies:
            c.wait()

    total = before[...].astype(jnp.float32)
    for i, s in enumerate((s0, s1, s2, s3)):
        total += jnp.dot(s[...], w[i], preferred_element_type=jnp.float32)
    o_ref[...] = total.astype(o_ref.dtype)


def output(at, own, got, before, wo, held, quarters, dtype, block=256):
    run, cols = got[0].shape
    d = wo.shape[1]
    steps = run // block
    rows = lambda c: pl.BlockSpec((block, c), lambda i, at: (i, 0))
    return pl.pallas_call(
        functools.partial(_output, quarters=quarters),
        grid_spec=pltpu.PrefetchScalarGridSpec(
            num_scalar_prefetch=1,
            grid=(steps,),
            in_specs=[pl.BlockSpec((block, cols), lambda i, at: (at[0] * steps + i, 0)), rows(cols), rows(cols), rows(cols), rows(d)] + [ANY] * 5,
            out_specs=rows(d),
            scratch_shapes=[pltpu.VMEM((4, cols, d), jnp.bfloat16), pltpu.SemaphoreType.DMA],
        ),
        out_shape=jax.ShapeDtypeStruct((run, d), dtype),
        compiler_params=pltpu.CompilerParams(dimension_semantics=("arbitrary",), vmem_limit_bytes=VMEM),
        cost_estimate=pl.CostEstimate(flops=8 * run * cols * d, transcendentals=0, bytes_accessed=8 * (run * cols + cols * d + run * d)),
        name="output",
    )(at, own, *got, before, wo, *held)


def solution(mesh):
    n, groups = mesh.shape["sp"], mesh.shape["dp"]

    def round_by(t, k):
        return lax.ppermute(t, "sp", [(i, (i + k) % n) for i in range(n)])

    def swap(t, k):
        return lax.ppermute(t, "dp", [(i, i ^ k) for i in range(groups)])

    def after(t, *others):
        return lax.optimization_barrier((t, *others))[0]

    def spread(pieces):
        near = jnp.stack(pieces)
        far = swap(near, 2)
        return near, far, swap(near, 1), swap(far, 1)

    def step(x, gain, wq, wk, wv, wo):
        own, d = x.shape
        me, quad = lax.axis_index("sp"), lax.rem(lax.axis_index("dp"), 4)
        part = wq.shape[0] // 4

        def columns(k):
            to = lax.rem(me + k + n, n)
            cut = lambda w: lax.dynamic_slice(w, (quad * part, to * (w.shape[1] // n)), (part, w.shape[1] // n))
            return jnp.concatenate([cut(wq), cut(wk), cut(wv)], 1)

        pieces = [round_by(columns(k), k) for k in (1, -1, 2)]
        half = own // 2
        top, low = normed(x[:half], gain), normed(x[half:], gain)
        before_top, after_low = round_by(top, 1), round_by(low, -1)
        before_low, after_top = round_by(low, 1), round_by(top, -1)
        far_top, far_low = round_by(before_top, 1), round_by(after_low, -1)
        held = spread(pieces)
        cos, sin = turns(own * n, THETA)

        def place(a, b):
            one = lambda k, low: 2 * lax.rem(me + k, n) + low
            return jnp.stack([one(*a), one(*b), me, quad]).astype(jnp.int32)

        weights = (wq, wk, wv)
        qkv = project(place((0, 0), (0, 1)), top, low, cos, sin, weights, held, None)
        qkv = project(place((3, 0), (1, 1)), before_top, after_low, cos, sin, weights, held, qkv)
        qkv = project(place((3, 1), (1, 0)), before_low, after_top, cos, sin, weights, held, qkv)
        qkv = project(place((2, 0), (2, 1)), far_top, far_low, cos, sin, weights, held, qkv)

        rows = wo.shape[0] // 4
        mine = after(lax.dynamic_slice(wo, (quad * rows, 0), (rows, d)), far_top, far_low)
        wo_held = spread([round_by(mine, k) for k in (1, -1, 2)])

        kb = 2
        total = x
        loops = qkv[1].shape[0] // kb
        at = jnp.stack([me, quad]).astype(jnp.int32)
        for i in range(loops):
            seen = attend(*qkv, i, kb)
            cut = lambda k: lax.dynamic_slice(seen, (lax.rem(me + k + n, n) * own, 0), (own, seen.shape[1]))
            got = [round_by(cut(k), k) for k in (1, -1, 2)]
            quarters = tuple(range(i * kb, i * kb + kb))
            total = output(at, seen, got, total, wo, wo_held, quarters, jnp.bfloat16 if i == loops - 1 else jnp.float32)
        return total

    tokens, whole = P(("dp", "sp"), None), P("sp", None)
    return jax.shard_map(
        step,
        mesh=mesh,
        in_specs=(tokens, P(None), whole, whole, whole, whole),
        out_specs=tokens,
        check_vma=False,
    )
```

```python
import functools

import jax
import jax.numpy as jnp
from jax import lax
from jax.experimental import pallas as pl
from jax.experimental.pallas import tpu as pltpu
import numpy as np
from jax.sharding import PartitionSpec as P

HEAD = 128
THETA = 10000
NEG = -1e30
HIDDEN = 2 * NEG
LOG2E = 1.4426950408889634
VMEM = 56 * 2**20
ANY = pl.BlockSpec(memory_space=pl.ANY)


def _dot(a, b, ca, cb):
    return lax.dot_general(a, b, (((ca,), (cb,)), ((), ())), preferred_element_type=jnp.float32)


def _first(x_ref, gain_ref, freq_ref, wq, wk, wv, q_out, k_out, v_out, held, w, cos_s, sin_s, put, own_sem, w_send, w_recv, far_send, far_recv,
           near_send, near_recv, a_send, a_recv, out_sem, *, n, wide):
    me, group = lax.axis_index("sp"), lax.axis_index("dp")
    right, left, over = lax.rem(me + 1, n), lax.rem(me + n - 1, n), lax.rem(me + 2, n)
    quad = lax.rem(group, 4)
    core, chip = lax.rem(quad, 2), lax.div(quad, 2)
    twin = {"dp": group + 1 - 2 * core}
    pal = {"dp": group + 2 - 4 * chip}
    rows, d = x_ref.shape
    depth = wq.shape[0]
    part = depth // 4
    nq, nk = q_out.shape[0] * HEAD, k_out.shape[0] * HEAD
    chunk = held.shape[1] // 2

    barrier = pltpu.get_barrier_semaphore()
    for to in ({"sp": right}, {"sp": left}, {"sp": over}, twin, pal):
        pl.semaphore_signal(barrier, inc=1, device_id=to, device_id_type=pl.DeviceIdType.MESH)
    pl.semaphore_wait(barrier, 5)

    def remote(src, dst, send, recv, to):
        return pltpu.make_async_remote_copy(src_ref=src, dst_ref=dst, send_sem=send, recv_sem=recv, device_id=to, device_id_type=pl.DeviceIdType.MESH)

    tall = pl.ds(me * depth + quad * part, part)
    mine = pl.ds(quad * part, part)
    direct = []
    for i, to in enumerate((right, left, over)):
        for j, (m, size, at) in enumerate(((wq, nq, 0), (wk, nk, nq), (wv, nk, nq + nk))):
            direct.append(remote(m.at[mine, pl.ds(to * size, size)], w.at[tall, pl.ds(at, size)], w_send.at[i, j], w_recv.at[i, j], {"sp": to}))
    for c in direct:
        c.start()
    all_own = pl.ds(me * depth, depth)
    local = [pltpu.make_async_copy(m.at[:, pl.ds(me * size, size)], w.at[all_own, pl.ds(at, size)], own_sem.at[j])
             for j, (m, size, at) in enumerate(((wq, nq, 0), (wk, nk, nq), (wv, nk, nq + nk)))]
    for c in local:
        c.start()

    def norm(i, _):
        at = pl.multiple_of(i * 128, 128)
        wide_x = x_ref[pl.ds(at, 128), :].astype(jnp.float32)
        scale = lax.rsqrt(jnp.mean(wide_x * wide_x, -1, keepdims=True) + 1e-6)
        per = 2 * chunk // 128
        held[lax.div(i, per), pl.ds(pl.multiple_of(lax.rem(i, per) * 128, 128), 128), :] = (wide_x * scale * gain_ref[...]).astype(jnp.bfloat16)

    lax.fori_loop(0, rows // 128, norm, None)

    def states(c):
        return held.at[c // 2, pl.ds(c % 2 * chunk, chunk), :]

    upper, lower = pl.ds(0, chunk), pl.ds(chunk, chunk)

    def table(i, _):
        at = pl.multiple_of(i * 128, 128)
        place = (lax.broadcasted_iota(jnp.int32, (128, HEAD), 0) + i * 128).astype(jnp.float32)
        angle = place * freq_ref[...]
        cos_s[pl.ds(at, 128), :] = jnp.cos(angle)
        first = lax.broadcasted_iota(jnp.int32, (128, HEAD), 1) < HEAD // 2
        sin_s[pl.ds(at, 128), :] = jnp.where(first, -1.0, 1.0) * jnp.sin(angle)

    sends = []
    for c in range(4):
        sends.append(remote(states(c), held.at[2 + c, upper, :], a_send.at[c, 0], a_recv.at[c, 0], {"sp": right}))
        sends.append(remote(states(3 - c), held.at[2 + c, lower, :], a_send.at[c, 1], a_recv.at[c, 1], {"sp": left}))
    for c in sends:
        c.start()
    lax.fori_loop(0, cos_s.shape[0] // 128, table, None)

    def rows_of(frm, quarter):
        return w.at[pl.ds(frm * depth + quarter * part, part), :]

    sources = (left, right, over)
    there = quad + 2 - 4 * chip
    fars, nears = [], []
    for i, frm in enumerate(sources):
        for j in range(3):
            direct[3 * i + j].wait_recv()
        fars.append(remote(rows_of(frm, quad), rows_of(frm, quad), far_send.at[i], far_recv.at[i], pal))
        nears.append(remote(rows_of(frm, quad), rows_of(frm, quad), near_send.at[0, i], near_recv.at[0, i], twin))
        fars[-1].start()
        nears[-1].start()
    for i, frm in enumerate(sources):
        fars[i].wait_recv()
        nears.append(remote(rows_of(frm, there), rows_of(frm, there), near_send.at[1, i], near_recv.at[1, i], twin))
        nears[-1].start()
    for c in nears:
        c.wait_recv()
    for c in local:
        c.wait()

    def outs(p, slot):
        early = p < 2
        passed = p >= 6
        a = jnp.where(early, me * 4 + 2 * p, jnp.where(passed, over * 4 + p - 6, left * 4 + p - 2))
        b = jnp.where(early, me * 4 + 2 * p + 1, jnp.where(passed, over * 4 + 9 - p, right * 4 + 5 - p))
        got = []
        for side, at in enumerate((a, b)):
            to = pl.ds(pl.multiple_of(at * chunk, chunk), chunk)
            frm = pl.ds(side * chunk, chunk)
            for j, (o, h0, h) in enumerate(((q_out, 0, nq // HEAD), (k_out, nq // HEAD, nk // HEAD), (v_out, (nq + nk) // HEAD, nk // HEAD))):
                got.append(pltpu.make_async_copy(put.at[slot, pl.ds(h0, h), frm, :], o.at[:, to, :], out_sem.at[slot, side, j]))
        return (a, b), got

    def arrival(p, side):
        return remote(held.at[p, pl.ds(side * chunk, chunk), :], held.at[p, pl.ds(side * chunk, chunk), :], a_send.at[p - 2, side], a_recv.at[p - 2, side],
                      {"sp": right if side == 0 else left})

    def pair(p, _):
        slot = lax.rem(p, 2)

        @pl.when(p >= 2)
        def _():
            for side in range(2):
                arrival(p, side).wait_recv()

        @pl.when((p >= 2) & (p < 4))
        def _():
            for side in range(2):
                half = pl.ds(side * chunk, chunk)
                remote(held.at[p, half, :], held.at[p + 4, half, :], a_send.at[p + 2, side], a_recv.at[p + 2, side], {"sp": left if side else right}).start()

        (a, b), copies = outs(p, slot)

        @pl.when(p >= 2)
        def _():
            for c in outs(p - 2, slot)[1]:
                c.wait()

        for at in range(0, w.shape[1], wide):
            got = jnp.dot(held[p], w[:, at : at + wide], preferred_element_type=jnp.float32).astype(jnp.bfloat16)
            for h in range(at, at + wide, HEAD):
                for side, first in enumerate((a, b)):
                    t = got[side * chunk : (side + 1) * chunk, h - at : h - at + HEAD]
                    if h < nq + nk:
                        t = t.astype(jnp.float32)
                        turn = pl.ds(pl.multiple_of(first * chunk, chunk), chunk)
                        t = (t * cos_s[turn, :] + pltpu.roll(t, HEAD // 2, 1) * sin_s[turn, :]).astype(jnp.bfloat16)
                    put[slot, h // HEAD, side * chunk : (side + 1) * chunk, :] = t
        for c in copies:
            c.start()

    lax.fori_loop(0, 8, pair, None)
    for p in (6, 7):
        for c in outs(p, p % 2)[1]:
            c.wait()
    for c in (*direct, *fars, *nears):
        c.wait_send()
    for p in range(2, 8):
        for side in range(2):
            arrival(p, side).wait_send()


def first(mesh, x, gain, wq, wk, wv):
    n = mesh.shape["sp"]
    rows, d = x.shape
    tokens, qh, kh = rows * n, wq.shape[1] // (n * HEAD), wk.shape[1] // (n * HEAD)
    heads = qh + 2 * kh
    freq = np.float32(THETA) ** (-np.arange(HEAD // 2, dtype=np.float32) / np.float32(HEAD // 2))
    freq = jnp.asarray(np.concatenate([freq, freq])[None])
    vmem = pl.BlockSpec(memory_space=pltpu.VMEM)
    dma = pltpu.SemaphoreType.DMA
    return pl.pallas_call(
        functools.partial(_first, n=n, wide=512),
        in_specs=[vmem, vmem, vmem, ANY, ANY, ANY],
        out_specs=[ANY] * 3,
        out_shape=[jax.ShapeDtypeStruct((h, tokens, HEAD), jnp.bfloat16) for h in (qh, kh, kh)],
        scratch_shapes=[
            pltpu.VMEM((8, rows // 2, d), jnp.bfloat16), pltpu.VMEM((d, heads * HEAD), jnp.bfloat16),
            pltpu.VMEM((tokens, HEAD), jnp.float32), pltpu.VMEM((tokens, HEAD), jnp.float32), pltpu.VMEM((2, heads, rows // 2, HEAD), jnp.bfloat16),
            dma((3,)), dma((3, 3)), dma((3, 3)), dma((3,)), dma((3,)), dma((2, 3)), dma((2, 3)), dma((6, 2)), dma((6, 2)), dma((2, 2, 3)),
        ],
        compiler_params=pltpu.CompilerParams(collective_id=0, has_side_effects=True, vmem_limit_bytes=VMEM),
        cost_estimate=pl.CostEstimate(flops=2 * tokens * d * heads * HEAD, transcendentals=0, bytes_accessed=2 * (d * heads * HEAD + tokens * (d + heads * HEAD))),
        name="first",
    )(x, gain.astype(jnp.float32)[None], freq, wq, wk, wv)


def _attend(q_ref, k_ref, v_ref, o_ref, top_s, mix_s, *, scale, bq, bk, wide):
    kb, d = k_ref.shape[0], k_ref.shape[2]
    g = q_ref.shape[0] // kb
    cols = g * bq
    iq = pl.program_id(0)
    e = scale * LOG2E
    pieces = [(i, at) for i in range(kb) for at in range(0, cols, wide)]
    top_s[...] = jnp.full(top_s.shape, NEG, jnp.float32)
    mix_s[...] = jnp.zeros(mix_s.shape, jnp.float32)
    ones = jnp.ones((8, bk), k_ref.dtype)

    def block(j, masked):
        here = pl.ds(pl.multiple_of(j * bk, bk), bk)
        scores = [_dot(k_ref[i, here, :], q_ref[g * i : g * i + g].reshape(cols, d)[at : at + wide, :], 1, 1) for i, at in pieces]
        weights, keeps = [], []
        for (i, at), s in zip(pieces, scores):
            if masked:
                gap = lax.rem(lax.broadcasted_iota(jnp.int32, (bk, wide), 1) + at, bq) - lax.broadcasted_iota(jnp.int32, (bk, wide), 0)
                s = jnp.where(gap >= j * bk - iq * bq, s, HIDDEN)
            old = top_s[i : i + 1, at : at + wide]
            top = jnp.maximum(old, s.max(axis=0, keepdims=True))
            top_s[i : i + 1, at : at + wide] = top
            weights.append(jnp.exp2((s - top) * e).astype(k_ref.dtype))
            keeps.append(jnp.exp2((old - top) * e))
        for (i, at), p, keep in zip(pieces, weights, keeps):
            values = jnp.concatenate([v_ref[i, here, :].T, ones], axis=0)
            mix_s[i, :, at : at + wide] = mix_s[i, :, at : at + wide] * keep + _dot(values, p, 1, 0)

    whole = iq * bq // bk
    lax.fori_loop(0, whole, lambda j, _: block(j, False), None)
    for n in range(max(bq // bk, 1)):
        block(whole + n, True)

    for i in range(kb):
        o = (mix_s[i, :d, :] * (1 / mix_s[i, d : d + 1, :])).T.astype(o_ref.dtype)
        for n in range(g):
            o_ref[:, (g * i + n) * d : (g * i + n + 1) * d] = o[n * bq : (n + 1) * bq]


def attend(q, k, v, first, kb, bq=512, bk=512, wide=512):
    h, tokens, d = q.shape
    g = h // k.shape[0]
    keys = pl.BlockSpec((kb, tokens, d), lambda i: (first, 0, 0))
    return pl.pallas_call(
        functools.partial(_attend, scale=d**-0.5, bq=bq, bk=bk, wide=wide),
        grid=(tokens // bq,),
        in_specs=[pl.BlockSpec((kb * g, bq, d), lambda i: (first, i, 0)), keys, keys],
        out_specs=pl.BlockSpec((bq, kb * g * d), lambda i: (i, 0)),
        out_shape=jax.ShapeDtypeStruct((tokens, kb * g * d), q.dtype),
        scratch_shapes=[pltpu.VMEM((kb, g * bq), jnp.float32), pltpu.VMEM((kb, d + 8, g * bq), jnp.float32)],
        compiler_params=pltpu.CompilerParams(dimension_semantics=("arbitrary",), vmem_limit_bytes=VMEM),
        cost_estimate=pl.CostEstimate(flops=4 * kb * g * tokens * tokens * d, transcendentals=kb * g * tokens * tokens // 2,
                                      bytes_accessed=2 * kb * tokens * d * (2 + 2 * g)),
        name="attend",
    )(q, k, v)


def _output(at_ref, s0, s1, s2, s3, before, wo, near, far, near2, far2, o_ref, w, sem, *, quarters):
    step = pl.program_id(0)
    depth = near.shape[1]

    @pl.when(step == 0)
    def _():
        quad = at_ref[1]
        copies = []
        for n, quarter in enumerate(quarters):
            copies.append(pltpu.make_async_copy(wo.at[pl.ds(quarter * depth, depth)], w.at[0, pl.ds(n * depth, depth)], sem))
            copies[-1].start()
            for i in range(3):
                put = w.at[1 + i, pl.ds(n * depth, depth)]
                for place, held in ((0, near), (2, far), (1, near2), (3, far2)):

                    @pl.when(jnp.bitwise_xor(quad, place) == quarter)
                    def _():
                        pltpu.make_async_copy(held.at[i], put, sem).start()

                copies.append(pltpu.make_async_copy(near.at[i], put, sem))
        for c in copies:
            c.wait()

    total = before[...].astype(jnp.float32)
    for i, s in enumerate((s0, s1, s2, s3)):
        total += jnp.dot(s[...], w[i], preferred_element_type=jnp.float32)
    o_ref[...] = total.astype(o_ref.dtype)


def output(at, own, got, before, wo, held, quarters, dtype, block=256):
    run, cols = got[0].shape
    d = wo.shape[1]
    steps = run // block
    rows = lambda c: pl.BlockSpec((block, c), lambda i, at: (i, 0))
    return pl.pallas_call(
        functools.partial(_output, quarters=quarters),
        grid_spec=pltpu.PrefetchScalarGridSpec(
            num_scalar_prefetch=1,
            grid=(steps,),
            in_specs=[pl.BlockSpec((block, cols), lambda i, at: (at[0] * steps + i, 0)), rows(cols), rows(cols), rows(cols), rows(d)] + [ANY] * 5,
            out_specs=rows(d),
            scratch_shapes=[pltpu.VMEM((4, cols, d), jnp.bfloat16), pltpu.SemaphoreType.DMA],
        ),
        out_shape=jax.ShapeDtypeStruct((run, d), dtype),
        compiler_params=pltpu.CompilerParams(dimension_semantics=("arbitrary",), vmem_limit_bytes=VMEM),
        cost_estimate=pl.CostEstimate(flops=8 * run * cols * d, transcendentals=0, bytes_accessed=8 * (run * cols + cols * d + run * d)),
        name="output",
    )(at, own, *got, before, wo, *held)


def solution(mesh):
    n, groups = mesh.shape["sp"], mesh.shape["dp"]

    def round_by(t, k):
        return lax.ppermute(t, "sp", [(i, (i + k) % n) for i in range(n)])

    def swap(t, k):
        return lax.ppermute(t, "dp", [(i, i ^ k) for i in range(groups)])

    def after(t, *others):
        return lax.optimization_barrier((t, *others))[0]

    def spread(pieces):
        near = jnp.stack(pieces)
        far = swap(near, 2)
        return near, far, swap(near, 1), swap(far, 1)

    def step(x, gain, wq, wk, wv, wo):
        own, d = x.shape
        me, quad = lax.axis_index("sp"), lax.rem(lax.axis_index("dp"), 4)
        qkv = first(mesh, x, gain, wq, wk, wv)

        rows = wo.shape[0] // 4
        mine = after(lax.dynamic_slice(wo, (quad * rows, 0), (rows, d)), qkv[0])
        wo_pieces = [round_by(mine, k) for k in (1, -1, 2)]

        kb = 2
        total = x
        loops = qkv[1].shape[0] // kb
        at = jnp.stack([me, quad]).astype(jnp.int32)
        for i in range(loops):
            seen = attend(*qkv, i, kb)
            if i == 0:
                wo_held = spread([after(t, seen) for t in wo_pieces])
            cut = lambda k: lax.dynamic_slice(seen, (lax.rem(me + k + n, n) * own, 0), (own, seen.shape[1]))
            got = [round_by(cut(k), k) for k in (1, -1, 2)]
            quarters = tuple(range(i * kb, i * kb + kb))
            total = output(at, seen, got, total, wo, wo_held, quarters, jnp.bfloat16 if i == loops - 1 else jnp.float32)
        return total

    tokens, whole = P(("dp", "sp"), None), P("sp", None)
    return jax.shard_map(
        step,
        mesh=mesh,
        in_specs=(tokens, P(None), whole, whole, whole, whole),
        out_specs=tokens,
        check_vma=False,
    )
```

```python
import functools

import jax
import jax.numpy as jnp
from jax import lax
from jax.experimental import pallas as pl
from jax.experimental.pallas import tpu as pltpu
import numpy as np
from jax.sharding import PartitionSpec as P

HEAD = 128
THETA = 10000
NEG = -1e30
HIDDEN = 2 * NEG
LOG2E = 1.4426950408889634
VMEM = 56 * 2**20
ANY = pl.BlockSpec(memory_space=pl.ANY)


def _dot(a, b, ca, cb):
    return lax.dot_general(a, b, (((ca,), (cb,)), ((), ())), preferred_element_type=jnp.float32)


def _first(x_ref, gain_ref, freq_ref, wq, wk, wv, q_out, k_out, v_out, held, w, cos_s, sin_s, put, own_sem, w_send, w_recv, far_send, far_recv,
           near_send, near_recv, a_send, a_recv, out_sem, *, n, wide):
    me, group = lax.axis_index("sp"), lax.axis_index("dp")
    right, left, over = lax.rem(me + 1, n), lax.rem(me + n - 1, n), lax.rem(me + 2, n)
    quad = lax.rem(group, 4)
    core, chip = lax.rem(quad, 2), lax.div(quad, 2)
    twin = {"dp": group + 1 - 2 * core}
    pal = {"dp": group + 2 - 4 * chip}
    rows, d = x_ref.shape
    depth = wq.shape[0]
    part = depth // 4
    nq, nk = q_out.shape[0] * HEAD, k_out.shape[0] * HEAD
    chunk = held.shape[1] // 2

    barrier = pltpu.get_barrier_semaphore()
    for to in ({"sp": right}, {"sp": left}, {"sp": over}, twin, pal):
        pl.semaphore_signal(barrier, inc=1, device_id=to, device_id_type=pl.DeviceIdType.MESH)
    pl.semaphore_wait(barrier, 5)

    def remote(src, dst, send, recv, to):
        return pltpu.make_async_remote_copy(src_ref=src, dst_ref=dst, send_sem=send, recv_sem=recv, device_id=to, device_id_type=pl.DeviceIdType.MESH)

    tall = pl.ds(me * depth + quad * part, part)
    mine = pl.ds(quad * part, part)
    direct = []
    for i, to in enumerate((right, left, over)):
        for j, (m, size, at) in enumerate(((wq, nq, 0), (wk, nk, nq), (wv, nk, nq + nk))):
            direct.append(remote(m.at[mine, pl.ds(to * size, size)], w.at[tall, pl.ds(at, size)], w_send.at[i, j], w_recv.at[i, j], {"sp": to}))
    for c in direct:
        c.start()
    all_own = pl.ds(me * depth, depth)
    local = [pltpu.make_async_copy(m.at[:, pl.ds(me * size, size)], w.at[all_own, pl.ds(at, size)], own_sem.at[j])
             for j, (m, size, at) in enumerate(((wq, nq, 0), (wk, nk, nq), (wv, nk, nq + nk)))]
    for c in local:
        c.start()

    def norm(i, _):
        at = pl.multiple_of(i * 128, 128)
        wide_x = x_ref[pl.ds(at, 128), :].astype(jnp.float32)
        scale = lax.rsqrt(jnp.mean(wide_x * wide_x, -1, keepdims=True) + 1e-6)
        per = 2 * chunk // 128
        held[lax.div(i, per), pl.ds(pl.multiple_of(lax.rem(i, per) * 128, 128), 128), :] = (wide_x * scale * gain_ref[...]).astype(jnp.bfloat16)

    lax.fori_loop(0, rows // 128, norm, None)

    def states(c):
        return held.at[c // 2, pl.ds(c % 2 * chunk, chunk), :]

    upper, lower = pl.ds(0, chunk), pl.ds(chunk, chunk)

    def table(i, _):
        at = pl.multiple_of(i * 128, 128)
        place = (lax.broadcasted_iota(jnp.int32, (128, HEAD), 0) + i * 128).astype(jnp.float32)
        angle = place * freq_ref[...]
        cos_s[pl.ds(at, 128), :] = jnp.cos(angle)
        first = lax.broadcasted_iota(jnp.int32, (128, HEAD), 1) < HEAD // 2
        sin_s[pl.ds(at, 128), :] = jnp.where(first, -1.0, 1.0) * jnp.sin(angle)

    sends = []
    for c in range(4):
        sends.append(remote(states(c), held.at[2 + c, upper, :], a_send.at[c, 0], a_recv.at[c, 0], {"sp": right}))
        sends.append(remote(states(3 - c), held.at[2 + c, lower, :], a_send.at[c, 1], a_recv.at[c, 1], {"sp": left}))
    for c in sends:
        c.start()
    lax.fori_loop(0, cos_s.shape[0] // 128, table, None)

    def rows_of(frm, quarter):
        return w.at[pl.ds(frm * depth + quarter * part, part), :]

    sources = (left, right, over)
    there = quad + 2 - 4 * chip
    fars, nears = [], []
    for i, frm in enumerate(sources):
        for j in range(3):
            direct[3 * i + j].wait_recv()
        fars.append(remote(rows_of(frm, quad), rows_of(frm, quad), far_send.at[i], far_recv.at[i], pal))
        nears.append(remote(rows_of(frm, quad), rows_of(frm, quad), near_send.at[0, i], near_recv.at[0, i], twin))
        fars[-1].start()
        nears[-1].start()
    for i, frm in enumerate(sources):
        fars[i].wait_recv()
        nears.append(remote(rows_of(frm, there), rows_of(frm, there), near_send.at[1, i], near_recv.at[1, i], twin))
        nears[-1].start()
    for c in nears:
        c.wait_recv()
    for c in local:
        c.wait()

    def outs(p, slot):
        early = p < 2
        passed = p >= 6
        a = jnp.where(early, me * 4 + 2 * p, jnp.where(passed, over * 4 + p - 6, left * 4 + p - 2))
        b = jnp.where(early, me * 4 + 2 * p + 1, jnp.where(passed, over * 4 + 9 - p, right * 4 + 5 - p))
        got = []
        for side, at in enumerate((a, b)):
            to = pl.ds(pl.multiple_of(at * chunk, chunk), chunk)
            frm = pl.ds(side * chunk, chunk)
            for j, (o, h0, h) in enumerate(((q_out, 0, nq // HEAD), (k_out, nq // HEAD, nk // HEAD), (v_out, (nq + nk) // HEAD, nk // HEAD))):
                got.append(pltpu.make_async_copy(put.at[slot, pl.ds(h0, h), frm, :], o.at[:, to, :], out_sem.at[slot, side, j]))
        return (a, b), got

    def arrival(p, side):
        return remote(held.at[p, pl.ds(side * chunk, chunk), :], held.at[p, pl.ds(side * chunk, chunk), :], a_send.at[p - 2, side], a_recv.at[p - 2, side],
                      {"sp": right if side == 0 else left})

    def pair(p, _):
        slot = lax.rem(p, 2)

        @pl.when(p >= 2)
        def _():
            for side in range(2):
                arrival(p, side).wait_recv()

        @pl.when((p >= 2) & (p < 4))
        def _():
            for side in range(2):
                half = pl.ds(side * chunk, chunk)
                remote(held.at[p, half, :], held.at[p + 4, half, :], a_send.at[p + 2, side], a_recv.at[p + 2, side], {"sp": left if side else right}).start()

        (a, b), copies = outs(p, slot)

        @pl.when(p >= 2)
        def _():
            for c in outs(p - 2, slot)[1]:
                c.wait()

        for at in range(0, w.shape[1], wide):
            got = jnp.dot(held[p], w[:, at : at + wide], preferred_element_type=jnp.float32).astype(jnp.bfloat16)
            for h in range(at, at + wide, HEAD):
                for side, first in enumerate((a, b)):
                    t = got[side * chunk : (side + 1) * chunk, h - at : h - at + HEAD]
                    if h < nq + nk:
                        t = t.astype(jnp.float32)
                        turn = pl.ds(pl.multiple_of(first * chunk, chunk), chunk)
                        t = (t * cos_s[turn, :] + pltpu.roll(t, HEAD // 2, 1) * sin_s[turn, :]).astype(jnp.bfloat16)
                    put[slot, h // HEAD, side * chunk : (side + 1) * chunk, :] = t
        for c in copies:
            c.start()

    lax.fori_loop(0, 8, pair, None)
    for p in (6, 7):
        for c in outs(p, p % 2)[1]:
            c.wait()
    for c in (*direct, *fars, *nears):
        c.wait_send()
    for p in range(2, 8):
        for side in range(2):
            arrival(p, side).wait_send()


def first(mesh, x, gain, wq, wk, wv):
    n = mesh.shape["sp"]
    rows, d = x.shape
    tokens, qh, kh = rows * n, wq.shape[1] // (n * HEAD), wk.shape[1] // (n * HEAD)
    heads = qh + 2 * kh
    freq = np.float32(THETA) ** (-np.arange(HEAD // 2, dtype=np.float32) / np.float32(HEAD // 2))
    freq = jnp.asarray(np.concatenate([freq, freq])[None])
    vmem = pl.BlockSpec(memory_space=pltpu.VMEM)
    dma = pltpu.SemaphoreType.DMA
    return pl.pallas_call(
        functools.partial(_first, n=n, wide=512),
        in_specs=[vmem, vmem, vmem, ANY, ANY, ANY],
        out_specs=[ANY] * 3,
        out_shape=[jax.ShapeDtypeStruct((h, tokens, HEAD), jnp.bfloat16) for h in (qh, kh, kh)],
        scratch_shapes=[
            pltpu.VMEM((8, rows // 2, d), jnp.bfloat16), pltpu.VMEM((d, heads * HEAD), jnp.bfloat16),
            pltpu.VMEM((tokens, HEAD), jnp.float32), pltpu.VMEM((tokens, HEAD), jnp.float32), pltpu.VMEM((2, heads, rows // 2, HEAD), jnp.bfloat16),
            dma((3,)), dma((3, 3)), dma((3, 3)), dma((3,)), dma((3,)), dma((2, 3)), dma((2, 3)), dma((6, 2)), dma((6, 2)), dma((2, 2, 3)),
        ],
        compiler_params=pltpu.CompilerParams(collective_id=0, has_side_effects=True, vmem_limit_bytes=VMEM),
        cost_estimate=pl.CostEstimate(flops=2 * tokens * d * heads * HEAD, transcendentals=0, bytes_accessed=2 * (d * heads * HEAD + tokens * (d + heads * HEAD))),
        name="first",
    )(x, gain.astype(jnp.float32)[None], freq, wq, wk, wv)


def _second(q, k, v, wo, x, y, k_s, v_s, q_s, x_s, got, wo_s, stage, top_s, mix_s, in_sem, q_sem, wo_own_sem, wo_send, wo_recv, far_send, far_recv,
            near_send, near_recv, seen_send, seen_recv, out_sem, *, n, scale, wide):
    me, group = lax.axis_index("sp"), lax.axis_index("dp")
    right, left, over = lax.rem(me + 1, n), lax.rem(me + n - 1, n), lax.rem(me + 2, n)
    quad = lax.rem(group, 4)
    core, chip = lax.rem(quad, 2), lax.div(quad, 2)
    twin = {"dp": group + 1 - 2 * core}
    pal = {"dp": group + 2 - 4 * chip}
    there = quad + 2 - 4 * chip
    kb, d = k_s.shape[0], k_s.shape[2]
    heads, run = q_s.shape[1], q_s.shape[2]
    g = heads // kb
    part = wo.shape[0] // 4
    e = scale * LOG2E

    barrier = pltpu.get_barrier_semaphore()
    for to in ({"sp": right}, {"sp": left}, {"sp": over}, twin, pal):
        pl.semaphore_signal(barrier, inc=1, device_id=to, device_id_type=pl.DeviceIdType.MESH)
    pl.semaphore_wait(barrier, 5)

    def remote(src, dst, send, recv, to):
        return pltpu.make_async_remote_copy(src_ref=src, dst_ref=dst, send_sem=send, recv_sem=recv, device_id=to, device_id_type=pl.DeviceIdType.MESH)

    def plan(i):
        odd = lax.rem(i, 2)
        owner = jnp.where(i < 4, jnp.where(odd == 0, over, 3 - over), jnp.where(i < 6, 3 - me, me))
        half = jnp.where(i < 4, jnp.where(odd == 0, lax.div(i, 2), 1 - lax.div(i, 2)), odd)
        return owner, half

    def fetch(i):
        owner, half = plan(i)
        at = pl.ds(pl.multiple_of((2 * owner + half) * run, run), run)
        return pltpu.make_async_copy(q.at[:, at, :], q_s.at[lax.rem(i, 2)], q_sem.at[lax.rem(i, 2)])

    def back(i):
        owner, half = plan(i)
        rel = lax.rem(owner - me + n, n)
        slot = jnp.where(rel == 1, 0, jnp.where(rel == 3, 1, 2))
        to = got.at[slot, pl.ds(pl.multiple_of(half * run, run), run), :]
        return remote(stage.at[lax.rem(i, 2)], to, seen_send.at[slot, half], seen_recv.at[slot, half], {"sp": owner})

    fetch(0).start()
    loads = [pltpu.make_async_copy(k, k_s, in_sem.at[0]), pltpu.make_async_copy(v, v_s, in_sem.at[1])]
    late = [pltpu.make_async_copy(x, x_s, in_sem.at[2]), pltpu.make_async_copy(wo, wo_s.at[3], wo_own_sem)]
    for c in loads:
        c.start()

    def rows_of(slot, quarter):
        return wo_s.at[slot, pl.ds(pl.multiple_of(quarter * part, part), part), :]

    direct = [remote(wo.at[pl.ds(pl.multiple_of(quad * part, part), part), :], rows_of(i, quad), wo_send.at[i], wo_recv.at[i], {"sp": to})
              for i, to in enumerate((right, left, over))]
    fars = [remote(rows_of(i, quad), rows_of(i, quad), far_send.at[i], far_recv.at[i], pal) for i in range(3)]
    nears = [[remote(rows_of(i, quarter), rows_of(i, quarter), near_send.at[m, i], near_recv.at[m, i], twin) for i in range(3)]
             for m, quarter in enumerate((quad, there))]
    for c in direct:
        c.start()
    for c in loads:
        c.wait()
    for c in late:
        c.start()

    pieces = [(i, m) for i in range(kb) for m in range(g)]
    ones = jnp.ones((8, run), k_s.dtype)

    def step(i, _):
        slot = lax.rem(i, 2)
        owner, half = plan(i)
        block_q = 2 * owner + half

        @pl.when(i < 7)
        def _():
            fetch(i + 1).start()

        for when, these in ((2, (0, 1)), (4, (2,))):

            @pl.when(i == when)
            def _():
                for m in these:
                    direct[m].wait_recv()
                    fars[m].start()
                    nears[0][m].start()

        @pl.when(i == 6)
        def _():
            for m in (0, 1):
                fars[m].wait_recv()
                nears[1][m].start()

        fetch(i).wait()
        top_s[...] = jnp.full(top_s.shape, NEG, jnp.float32)
        mix_s[...] = jnp.zeros(mix_s.shape, jnp.float32)

        def block(j, masked):
            here = pl.ds(pl.multiple_of(j * run, run), run)
            scores = [_dot(k_s[i, here, :], q_s[slot, g * i + m], 1, 1) for i, m in pieces]
            if masked:
                ok = lax.broadcasted_iota(jnp.int32, (run, run), 1) >= lax.broadcasted_iota(jnp.int32, (run, run), 0)
            weights, keeps = [], []
            for (i, m), s in zip(pieces, scores):
                if masked:
                    s = jnp.where(ok, s, HIDDEN)
                old = top_s[i : i + 1, m * run : (m + 1) * run]
                top = jnp.maximum(old, s.max(axis=0, keepdims=True))
                top_s[i : i + 1, m * run : (m + 1) * run] = top
                weights.append(jnp.exp2((s - top) * e).astype(k_s.dtype))
                keeps.append(jnp.exp2((old - top) * e))
            for (i, m), p, keep in zip(pieces, weights, keeps):
                values = jnp.concatenate([v_s[i, here, :].T, ones], axis=0)
                mix_s[i, :, m * run : (m + 1) * run] = mix_s[i, :, m * run : (m + 1) * run] * keep + _dot(values, p, 1, 0)

        lax.fori_loop(0, block_q, lambda j, _: block(j, False), None)
        block(block_q, True)

        @pl.when((i >= 2) & (i < 6))
        def _():
            back(i - 2).wait_send()

        def store(put):
            for i, m in pieces:
                o = mix_s[i, :d, m * run : (m + 1) * run] * (1 / mix_s[i, d : d + 1, m * run : (m + 1) * run])
                put((g * i + m) * d, o.T.astype(stage.dtype))

        @pl.when(i < 6)
        def _():
            def put(at, o):
                stage[slot, :, at : at + d] = o

            store(put)
            back(i).start()

        @pl.when(i >= 6)
        def _():
            def put(at, o):
                got[3, pl.ds(pl.multiple_of(half * run, run), run), at : at + d] = o

            store(put)

    lax.fori_loop(0, 8, step, None)

    fars[2].wait_recv()
    nears[1][2].start()
    for c in late:
        c.wait()
    for m in range(2):
        for c in nears[m]:
            c.wait_recv()

    tile = 256

    def done(t):
        at = pl.ds(pl.multiple_of(t * tile, tile), tile)
        return pltpu.make_async_copy(x_s.at[at, :], y.at[at, :], out_sem.at[t])

    for half in range(2):
        for m in range(3):
            arrived = got.at[m, pl.ds(half * run, run), :]
            remote(arrived, arrived, seen_send.at[m, half], seen_recv.at[m, half], {"sp": (left, right, over)[m]}).wait_recv()

        def finish(t, _):
            at = pl.ds(pl.multiple_of(t * tile, tile), tile)
            for c in range(0, x_s.shape[1], wide):
                total = jnp.dot(got[0, at, :], wo_s[0, :, c : c + wide], preferred_element_type=jnp.float32)
                for m in range(1, 4):
                    total += jnp.dot(got[m, at, :], wo_s[m, :, c : c + wide], preferred_element_type=jnp.float32)
                x_s[at, c : c + wide] = (x_s[at, c : c + wide].astype(jnp.float32) + total).astype(x_s.dtype)
            done(t).start()

        lax.fori_loop(half * (run // tile), (half + 1) * (run // tile), finish, None)

    for t in range(2 * run // tile):
        done(t).wait()
    for i in (4, 5):
        back(i).wait_send()
    for c in (*direct, *fars, *nears[0], *nears[1]):
        c.wait_send()


def second(mesh, q, k, v, wo, x):
    n = mesh.shape["sp"]
    heads, tokens, hd = q.shape
    kb = k.shape[0]
    g = heads // kb
    rows, d = x.shape
    run = rows // 2
    bf, dma = jnp.bfloat16, pltpu.SemaphoreType.DMA
    return pl.pallas_call(
        functools.partial(_second, n=n, scale=hd**-0.5, wide=512),
        in_specs=[ANY] * 5,
        out_specs=ANY,
        out_shape=jax.ShapeDtypeStruct((rows, d), bf),
        scratch_shapes=[
            pltpu.VMEM(k.shape, bf), pltpu.VMEM(v.shape, bf), pltpu.VMEM((2, heads, run, hd), bf), pltpu.VMEM((rows, d), bf),
            pltpu.VMEM((4, rows, heads * hd), bf), pltpu.VMEM((4, *wo.shape), bf), pltpu.VMEM((2, run, heads * hd), bf),
            pltpu.VMEM((kb, g * run), jnp.float32), pltpu.VMEM((kb, hd + 8, g * run), jnp.float32),
            dma((3,)), dma((2,)), dma, dma((3,)), dma((3,)), dma((3,)), dma((3,)), dma((2, 3)), dma((2, 3)), dma((3, 2)), dma((3, 2)), dma((4,)),
        ],
        compiler_params=pltpu.CompilerParams(collective_id=1, has_side_effects=True, vmem_limit_bytes=67043328),
        cost_estimate=pl.CostEstimate(flops=2 * heads * tokens * tokens * hd + 2 * rows * n * heads * hd * d, transcendentals=heads * tokens * tokens // 2,
                                      bytes_accessed=2 * (2 * q.size + 2 * k.size + 4 * wo.size + 2 * x.size)),
        name="second",
    )(q, k, v, wo, x)


def solution(mesh):
    def step(x, gain, wq, wk, wv, wo):
        q, k, v = first(mesh, x, gain, wq, wk, wv)
        return second(mesh, q, k, v, wo, x)

    tokens, whole = P(("dp", "sp"), None), P("sp", None)
    return jax.shard_map(
        step,
        mesh=mesh,
        in_specs=(tokens, P(None), whole, whole, whole, whole),
        out_specs=tokens,
        check_vma=False,
    )
```

```python
import functools

import jax
import jax.numpy as jnp
from jax import lax
from jax.experimental import pallas as pl
from jax.experimental.pallas import tpu as pltpu
import numpy as np
from jax.sharding import PartitionSpec as P

HEAD = 128
THETA = 10000
NEG = -1e30
HIDDEN = 2 * NEG
LOG2E = 1.4426950408889634
VMEM = 56 * 2**20
ANY = pl.BlockSpec(memory_space=pl.ANY)


def _dot(a, b, ca, cb):
    return lax.dot_general(a, b, (((ca,), (cb,)), ((), ())), preferred_element_type=jnp.float32)


def _layer(x, gain_ref, freq_ref, wq, wk, wv, wo, y, held, w, q_s, k_s, v_s, wo_s, cos_s, sin_s, top_s, mix_s, x_sem, own_sem, w_send, w_recv,
           w_far_send, w_far_recv, w_near_send, w_near_recv, a_send, a_recv, o_send, o_recv, o_far_send, o_far_recv, o_near_send, o_near_recv,
           seen_send, seen_recv, out_sem, ready, *, n, scale, wide, ahead):
    me, group = lax.axis_index("sp"), lax.axis_index("dp")
    right, left, over = lax.rem(me + 1, n), lax.rem(me + n - 1, n), lax.rem(me + 2, n)
    quad = lax.rem(group, 4)
    core, chip = lax.rem(quad, 2), lax.div(quad, 2)
    twin = {"dp": group + 1 - 2 * core}
    pal = {"dp": group + 2 - 4 * chip}
    there = quad + 2 - 4 * chip
    rows, d = x.shape
    run, chunk = rows // 2, rows // 4
    heads, kb = q_s.shape[0], k_s.shape[0]
    g = heads // kb
    nq, nk = heads * HEAD, kb * HEAD
    e = scale * LOG2E

    fill = [pltpu.make_async_copy(x.at[pl.ds(i * run, run), :], held.at[i], x_sem.at[i]) for i in range(2)]
    for c in fill:
        c.start()
    barrier = pltpu.get_barrier_semaphore()
    for to in ({"sp": right}, {"sp": left}, {"sp": over}, twin, pal):
        pl.semaphore_signal(barrier, inc=1, device_id=to, device_id_type=pl.DeviceIdType.MESH)
    pl.semaphore_wait(barrier, 5)

    def remote(src, dst, send, recv, to):
        return pltpu.make_async_remote_copy(src_ref=src, dst_ref=dst, send_sem=send, recv_sem=recv, device_id=to, device_id_type=pl.DeviceIdType.MESH)

    depth = wq.shape[0]
    part = depth // 4
    tall = pl.ds(me * depth + quad * part, part)
    mine = pl.ds(quad * part, part)
    kinds = ((wq, nq, 0), (wk, nk, nq), (wv, nk, nq + nk))
    direct = []
    for i, to in enumerate((right, left, over)):
        for j, (m, size, at) in enumerate(kinds):
            direct.append(remote(m.at[mine, pl.ds(to * size, size)], w.at[tall, pl.ds(at, size)], w_send.at[i, j], w_recv.at[i, j], {"sp": to}))
    for c in direct:
        c.start()
    all_own = pl.ds(me * depth, depth)
    local = [pltpu.make_async_copy(m.at[:, pl.ds(me * size, size)], w.at[all_own, pl.ds(at, size)], own_sem.at[j])
             for j, (m, size, at) in enumerate(kinds)]
    for c in fill:
        c.wait()

    def norm(i, _):
        per = run // 128
        at = pl.ds(pl.multiple_of(lax.rem(i, per) * 128, 128), 128)
        wide_x = held[lax.div(i, per), at, :].astype(jnp.float32)
        rms = lax.rsqrt(jnp.mean(wide_x * wide_x, -1, keepdims=True) + 1e-6)
        held[lax.div(i, per), at, :] = (wide_x * rms * gain_ref[...].astype(jnp.float32)).astype(jnp.bfloat16)

    lax.fori_loop(0, rows // 128, norm, None)
    for c in local:
        c.start()

    def states(c):
        return held.at[c // 2, pl.ds(c % 2 * chunk, chunk), :]

    upper, lower = pl.ds(0, chunk), pl.ds(chunk, chunk)
    sends = []
    for c in range(4):
        sends.append(remote(states(c), held.at[2 + c, upper, :], a_send.at[c, 0], a_recv.at[c, 0], {"sp": right}))
        sends.append(remote(states(3 - c), held.at[2 + c, lower, :], a_send.at[c, 1], a_recv.at[c, 1], {"sp": left}))
    for c in sends:
        c.start()

    def w_rows(frm, quarter):
        return w.at[pl.ds(frm * depth + quarter * part, part), :]

    sources = (left, right, over)
    fars, nears = [], []
    for i, frm in enumerate(sources):
        for j in range(3):
            direct[3 * i + j].wait_recv()
        fars.append(remote(w_rows(frm, quad), w_rows(frm, quad), w_far_send.at[i], w_far_recv.at[i], pal))
        nears.append(remote(w_rows(frm, quad), w_rows(frm, quad), w_near_send.at[0, i], w_near_recv.at[0, i], twin))
        fars[-1].start()
        nears[-1].start()
    for i, frm in enumerate(sources):
        fars[i].wait_recv()
        nears.append(remote(w_rows(frm, there), w_rows(frm, there), w_near_send.at[1, i], w_near_recv.at[1, i], twin))
        nears[-1].start()
    for c in nears:
        c.wait_recv()
    for c in local:
        c.wait()

    slab = wo.shape[0] // 4

    def o_rows(slot, quarter):
        return wo_s.at[slot, pl.ds(pl.multiple_of(quarter * slab, slab), slab), :]

    o_direct = [remote(wo.at[pl.ds(pl.multiple_of(quad * slab, slab), slab), :], o_rows(i, quad), o_send.at[i], o_recv.at[i], {"sp": to})
                for i, to in enumerate((right, left, over))]
    o_fars = [remote(o_rows(i, quad), o_rows(i, quad), o_far_send.at[i], o_far_recv.at[i], pal) for i in range(3)]
    o_nears = [[remote(o_rows(i, quarter), o_rows(i, quarter), o_near_send.at[m, i], o_near_recv.at[m, i], twin) for i in range(3)]
               for m, quarter in enumerate((quad, there))]

    def arrival(p, side):
        half = pl.ds(side * chunk, chunk)
        return remote(held.at[p, half, :], held.at[p, half, :], a_send.at[p - 2, side], a_recv.at[p - 2, side], {"sp": left if side else right})

    def pair(p, _):
        early, passed = p < 2, p >= 6
        firsts = (jnp.where(early, me * 4 + 2 * p, jnp.where(passed, over * 4 + p - 6, left * 4 + p - 2)),
                  jnp.where(early, me * 4 + 2 * p + 1, jnp.where(passed, over * 4 + 9 - p, right * 4 + 5 - p)))
        for side, at in enumerate(firsts):
            place = (lax.broadcasted_iota(jnp.int32, (chunk, HEAD), 0) + at * chunk).astype(jnp.float32)
            angle = place * freq_ref[...]
            cos_s[side * chunk : (side + 1) * chunk, :] = jnp.cos(angle)
            sign = jnp.where(lax.broadcasted_iota(jnp.int32, (chunk, HEAD), 1) < HEAD // 2, -1.0, 1.0)
            sin_s[side * chunk : (side + 1) * chunk, :] = sign * jnp.sin(angle)

        @pl.when(p >= 2)
        def _():
            for side in range(2):
                arrival(p, side).wait_recv()

        @pl.when((p >= 2) & (p < 4))
        def _():
            for side in range(2):
                half = pl.ds(side * chunk, chunk)
                remote(held.at[p, half, :], held.at[p + 4, half, :], a_send.at[p + 2, side], a_recv.at[p + 2, side], {"sp": left if side else right}).start()

        @pl.when(p == 6)
        def _():
            for c in o_direct:
                c.start()

        for at in range(0, w.shape[1], wide):
            got = jnp.dot(held[p], w[:, at : at + wide], preferred_element_type=jnp.float32).astype(jnp.bfloat16)
            for h in range(at, at + wide, HEAD):
                t = got[:, h - at : h - at + HEAD]
                if h < nq + nk:
                    t = t.astype(jnp.float32)
                    t = (t * cos_s[...] + pltpu.roll(t, HEAD // 2, 1) * sin_s[...]).astype(jnp.bfloat16)
                for side, first in enumerate(firsts):
                    to = pl.ds(pl.multiple_of(first * chunk, chunk), chunk)
                    half = t[side * chunk : (side + 1) * chunk]
                    if h < nq:
                        q_s[h // HEAD, to, :] = half
                    elif h < nq + nk:
                        k_s[(h - nq) // HEAD, to, :] = half
                    else:
                        v_s[(h - nq - nk) // HEAD, to, :] = half

    lax.fori_loop(0, 8, pair, None)
    for c in (*direct, *fars, *nears):
        c.wait_send()
    for p in range(2, 8):
        for side in range(2):
            arrival(p, side).wait_send()
    for to in (right, left, over):
        pl.semaphore_signal(ready, inc=1, device_id={"sp": to}, device_id_type=pl.DeviceIdType.MESH)
    fill = [pltpu.make_async_copy(x.at[pl.ds(i * run, run), :], held.at[3 + i], x_sem.at[i]) for i in range(2)]
    fill += [pltpu.make_async_copy(wo.at[pl.ds(i * run, run), :], held.at[5 + i], own_sem.at[i]) for i in range(2)]
    for c in fill:
        c.start()

    def plan(i):
        odd = lax.rem(i, 2)
        owner = jnp.where(i < 4, jnp.where(odd == 0, over, 3 - over), jnp.where(i < 6, 3 - me, me))
        half = jnp.where(i < 4, jnp.where(odd == 0, lax.div(i, 2), 1 - lax.div(i, 2)), odd)
        return owner, half

    def seen_at(slot, half):
        row, col = lax.div(slot, 2) * rows + half * run, lax.rem(slot, 2) * nq
        return w.at[pl.ds(pl.multiple_of(row, run), run), pl.ds(pl.multiple_of(col, nq), nq)]

    def staged(i):
        return held.at[lax.div(i, 2), :, pl.ds(pl.multiple_of(lax.rem(i, 2) * nq, nq), nq)]

    def back(i):
        owner, half = plan(i)
        rel = lax.rem(owner - me + n, n)
        slot = jnp.where(rel == 1, 0, jnp.where(rel == 3, 1, 2))
        return remote(staged(i), seen_at(slot, half), seen_send.at[slot, half], seen_recv.at[slot, half], {"sp": owner})

    pieces = [(i, m) for i in range(kb) for m in range(g)]
    ones = jnp.ones((8, run), k_s.dtype)

    def step(i, _):
        owner, half = plan(i)
        block_q = 2 * owner + half

        for when, these in ((2, (0, 1)), (4, (2,))):

            @pl.when(i == when)
            def _():
                for m in these:
                    o_direct[m].wait_recv()
                    o_fars[m].start()
                    o_nears[0][m].start()

        @pl.when(i == 7)
        def _():
            for m in (0, 1):
                o_fars[m].wait_recv()
                o_nears[1][m].start()

        top_s[...] = jnp.full(top_s.shape, NEG, jnp.float32)
        mix_s[...] = jnp.zeros(mix_s.shape, jnp.float32)
        queries = pl.ds(pl.multiple_of(block_q * run, run), run)

        def block(j, masked):
            here = pl.ds(pl.multiple_of(j * run, run), run)
            if masked:
                ok = lax.broadcasted_iota(jnp.int32, (run, run), 1) >= lax.broadcasted_iota(jnp.int32, (run, run), 0)

            def score(i, m):
                return _dot(k_s[i, here, :], q_s[g * i + m, queries, :], 1, 1)

            scores = [score(*piece) for piece in pieces[:ahead]]
            for at, (i, m) in enumerate(pieces):
                if at + ahead < len(pieces):
                    scores.append(score(*pieces[at + ahead]))
                s = jnp.where(ok, scores[at], HIDDEN) if masked else scores[at]
                own = slice(m * run, (m + 1) * run)
                old = top_s[i : i + 1, own]
                top = jnp.maximum(old, s.max(axis=0, keepdims=True))
                top_s[i : i + 1, own] = top
                p = jnp.exp2((s - top) * e).astype(k_s.dtype)
                values = jnp.concatenate([v_s[i, here, :].T, ones], axis=0)
                mix_s[i, :, own] = mix_s[i, :, own] * jnp.exp2((old - top) * e) + _dot(values, p, 1, 0)

        lax.fori_loop(0, block_q, lambda j, _: block(j, False), None)
        block(block_q, True)

        def store(put):
            for i, m in pieces:
                o = mix_s[i, :HEAD, m * run : (m + 1) * run] * (1 / mix_s[i, HEAD : HEAD + 1, m * run : (m + 1) * run])
                put((g * i + m) * HEAD, o.T.astype(held.dtype))

        @pl.when(i == 0)
        def _():
            pl.semaphore_wait(ready, 3)

        @pl.when(i < 6)
        def _():
            def put(at, o):
                staged(i)[:, at : at + HEAD] = o

            store(put)
            back(i).start()

        @pl.when(i >= 6)
        def _():
            def put(at, o):
                w[pl.ds(pl.multiple_of(rows + half * run, run), run), nq + at : nq + at + HEAD] = o

            store(put)

    lax.fori_loop(0, 8, step, None)

    o_fars[2].wait_recv()
    o_nears[1][2].start()
    for c in fill:
        c.wait()
    for m in range(2):
        for c in o_nears[m]:
            c.wait_recv()

    tile = 256

    def done(t):
        per = run // tile
        at = pl.ds(pl.multiple_of(lax.rem(t, per) * tile, tile), tile)
        return pltpu.make_async_copy(held.at[3 + lax.div(t, per), at, :], y.at[pl.ds(pl.multiple_of(t * tile, tile), tile), :], out_sem.at[t])

    for half in range(2):
        for m in range(3):
            remote(seen_at(m, half), seen_at(m, half), seen_send.at[m, half], seen_recv.at[m, half], {"sp": (left, right, over)[m]}).wait_recv()

        def finish(t, _):
            at = pl.ds(pl.multiple_of(t * tile, tile), tile)
            for c in range(0, d, wide):
                total = None
                for m in range(4):
                    tokens = pl.ds(pl.multiple_of(m // 2 * rows + half * run + t * tile, tile), tile)
                    if m < 3:
                        parts = [(w[tokens, m % 2 * nq : (m % 2 + 1) * nq], wo_s[m, :, c : c + wide])]
                    else:
                        parts = [(w[tokens, nq + k * run : nq + (k + 1) * run], held[5 + k, :, c : c + wide]) for k in range(2)]
                    for seen, weight in parts:
                        got = jnp.dot(seen, weight, preferred_element_type=jnp.float32)
                        total = got if total is None else total + got
                held[3 + half, at, c : c + wide] = (held[3 + half, at, c : c + wide].astype(jnp.float32) + total).astype(held.dtype)
            done(half * (run // tile) + t).start()

        lax.fori_loop(0, run // tile, finish, None)

    for t in range(rows // tile):
        done(t).wait()
    for i in range(6):
        back(i).wait_send()
    for c in (*o_direct, *o_fars, *o_nears[0], *o_nears[1]):
        c.wait_send()


def layer(mesh, x, gain, wq, wk, wv, wo):
    n = mesh.shape["sp"]
    rows, d = x.shape
    tokens, heads, kb = rows * n, wq.shape[1] // (n * HEAD), wk.shape[1] // (n * HEAD)
    g, run = heads // kb, rows // 2
    freq = np.float32(THETA) ** (-np.arange(HEAD // 2, dtype=np.float32) / np.float32(HEAD // 2))
    freq = jnp.asarray(np.concatenate([freq, freq])[None])
    vmem = pl.BlockSpec(memory_space=pltpu.VMEM)
    bf, dma = jnp.bfloat16, pltpu.SemaphoreType.DMA
    return pl.pallas_call(
        functools.partial(_layer, n=n, scale=HEAD**-0.5, wide=512, ahead=4),
        in_specs=[ANY, vmem, vmem, ANY, ANY, ANY, ANY],
        out_specs=ANY,
        out_shape=jax.ShapeDtypeStruct((rows, d), bf),
        scratch_shapes=[
            pltpu.VMEM((8, run, d), bf), pltpu.VMEM((d, (heads + 2 * kb) * HEAD), bf), pltpu.VMEM((heads, tokens, HEAD), bf),
            pltpu.VMEM((kb, tokens, HEAD), bf), pltpu.VMEM((kb, tokens, HEAD), bf), pltpu.VMEM((3, *wo.shape), bf),
            pltpu.VMEM((run, HEAD), jnp.float32), pltpu.VMEM((run, HEAD), jnp.float32),
            pltpu.VMEM((kb, g * run), jnp.float32), pltpu.VMEM((kb, HEAD + 8, g * run), jnp.float32),
            dma((2,)), dma((3,)), dma((3, 3)), dma((3, 3)), dma((3,)), dma((3,)), dma((2, 3)), dma((2, 3)), dma((6, 2)), dma((6, 2)),
            dma((3,)), dma((3,)), dma((3,)), dma((3,)), dma((2, 3)), dma((2, 3)), dma((3, 2)), dma((3, 2)), dma((4,)), pltpu.SemaphoreType.REGULAR,
        ],
        compiler_params=pltpu.CompilerParams(collective_id=0, has_side_effects=True, vmem_limit_bytes=67043328),
        cost_estimate=pl.CostEstimate(flops=2 * heads * tokens * tokens * HEAD + 6 * tokens * d * heads * HEAD, transcendentals=heads * tokens * tokens // 2,
                                      bytes_accessed=2 * (2 * x.size + 4 * wo.size)),
        name="layer",
    )(x, gain[None], freq, wq, wk, wv, wo)


def solution(mesh):
    tokens, whole = P(("dp", "sp"), None), P("sp", None)
    return jax.shard_map(
        functools.partial(layer, mesh),
        mesh=mesh,
        in_specs=(tokens, P(None), whole, whole, whole, whole),
        out_specs=tokens,
        check_vma=False,
    )
```

```python
import functools

import jax
import jax.numpy as jnp
from jax import lax
from jax.experimental import pallas as pl
from jax.experimental.pallas import tpu as pltpu
import numpy as np
from jax.sharding import PartitionSpec as P

HEAD = 128
THETA = 10000
NEG = -1e30
HIDDEN = 2 * NEG
LOG2E = 1.4426950408889634
ANY = pl.BlockSpec(memory_space=pl.ANY)
ORDER = (("early", 1), ("late", 1), ("late", 0), ("early", 0), ("over", 0), ("over", 1), ("own", 0), ("own", 1))


def _dot(a, b, ca, cb):
    return lax.dot_general(a, b, (((ca,), (cb,)), ((), ())), preferred_element_type=jnp.float32)


def _layer(x, gain_ref, freq_ref, wq, wk, wv, wo, y, held, w, q_s, k_s, v_s, wo_s, cos_s, sin_s, top_s, mix_s, w_via, wo_via, x_sem, own_sem, w_send, w_recv,
           via_send, via_recv,
           w_far_send, w_far_recv, w_near_send, w_near_recv, a_send, a_recv, o_send, o_recv, o_far_send, o_far_recv, o_near_send, o_near_recv,
           seen_send, seen_recv, out_sem, ready, *, n, scale, wide, ahead):
    me, group = lax.axis_index("sp"), lax.axis_index("dp")
    right, left, over = lax.rem(me + 1, n), lax.rem(me + n - 1, n), lax.rem(me + 2, n)
    quad = lax.rem(group, 4)
    core, chip = lax.rem(quad, 2), lax.div(quad, 2)
    twin = {"dp": group + 1 - 2 * core}
    pal = {"dp": group + 2 - 4 * chip}
    there = quad + 2 - 4 * chip
    rows, d = x.shape
    run, chunk = rows // 2, rows // 4
    tile = 256
    heads, kb = q_s.shape[0], k_s.shape[0]
    g = heads // kb
    nq, nk = heads * HEAD, kb * HEAD
    e = scale * LOG2E

    fill = [pltpu.make_async_copy(x.at[pl.ds(i * run, run), :], held.at[i], x_sem.at[i]) for i in range(2)]
    for c in fill:
        c.start()
    barrier = pltpu.get_barrier_semaphore()
    for to in ({"sp": right}, {"sp": left}, {"sp": over}, twin, pal):
        pl.semaphore_signal(barrier, inc=1, device_id=to, device_id_type=pl.DeviceIdType.MESH)
    pl.semaphore_wait(barrier, 5)

    def remote(src, dst, send, recv, to):
        return pltpu.make_async_remote_copy(src_ref=src, dst_ref=dst, send_sem=send, recv_sem=recv, device_id=to, device_id_type=pl.DeviceIdType.MESH)

    depth = wq.shape[0]
    part = depth // 4
    kinds = ((wq, nq, 0), (wk, nk, nq), (wv, nk, nq + nk))
    direct = []
    for i, to in enumerate((right, left)):
        by = pl.ds(quad * part + i * (part // 2), part // 2)
        for j, (m, size, at) in enumerate(kinds):
            direct.append(remote(m.at[by, pl.ds(over * size, size)], w_via.at[i, :, pl.ds(at, size)], w_send.at[2 + i, j], w_recv.at[2 + i, j], {"sp": to}))
    for i, to in enumerate((right, left)):
        mine, there_at = pl.ds(quad * part, part), pl.ds(me * depth + quad * part, part)
        for j, (m, size, at) in enumerate(kinds):
            direct.append(remote(m.at[mine, pl.ds(to * size, size)], w.at[there_at, pl.ds(at, size)], w_send.at[i, j], w_recv.at[i, j], {"sp": to}))
    for c in direct:
        c.start()
    all_own = pl.ds(me * depth, depth)
    local = [pltpu.make_async_copy(m.at[:, pl.ds(me * size, size)], w.at[all_own, pl.ds(at, size)], own_sem.at[j])
             for j, (m, size, at) in enumerate(kinds)]
    for c in fill:
        c.wait()

    def norm(i, _):
        per = run // 128
        at = pl.ds(pl.multiple_of(lax.rem(i, per) * 128, 128), 128)
        wide_x = held[lax.div(i, per), at, :].astype(jnp.float32)
        rms = lax.rsqrt(jnp.mean(wide_x * wide_x, -1, keepdims=True) + 1e-6)
        held[lax.div(i, per), at, :] = (wide_x * rms * gain_ref[...].astype(jnp.float32)).astype(jnp.bfloat16)

    lax.fori_loop(0, rows // 128, norm, None)
    for c in local:
        c.start()

    def states(c):
        return held.at[c // 2, pl.ds(c % 2 * chunk, chunk), :]

    upper, lower = pl.ds(0, chunk), pl.ds(chunk, chunk)
    sends = []
    for c in range(4):
        sends.append(remote(states(c), held.at[2 + c, upper, :], a_send.at[c, 0], a_recv.at[c, 0], {"sp": right}))
        sends.append(remote(states(3 - c), held.at[2 + c, lower, :], a_send.at[c, 1], a_recv.at[c, 1], {"sp": left}))
    for c in sends[:2]:
        c.start()
    passed_on = []
    for i, (frm, to) in enumerate(((left, right), (right, left))):
        for j in range(3):
            direct[3 * i + j].wait_recv()
        put = w.at[pl.ds(frm * depth + quad * part + i * (part // 2), part // 2), :]
        passed_on.append(remote(w_via.at[i], put, via_send.at[i], via_recv.at[i], {"sp": to}))
        passed_on[-1].start()
    for c in sends[2:]:
        c.start()

    def w_rows(frm, quarter):
        return w.at[pl.ds(frm * depth + quarter * part, part), :]

    sources = (left, right, over)
    fars, nears = [], []
    for i, frm in enumerate(sources):
        if i < 2:
            for j in range(3):
                direct[6 + 3 * i + j].wait_recv()
        else:
            for c in passed_on:
                c.wait_recv()
        fars.append(remote(w_rows(frm, quad), w_rows(frm, quad), w_far_send.at[i], w_far_recv.at[i], pal))
        nears.append(remote(w_rows(frm, quad), w_rows(frm, quad), w_near_send.at[0, i], w_near_recv.at[0, i], twin))
        fars[-1].start()
        nears[-1].start()
    for i, frm in enumerate(sources):
        fars[i].wait_recv()
        nears.append(remote(w_rows(frm, there), w_rows(frm, there), w_near_send.at[1, i], w_near_recv.at[1, i], twin))
        nears[-1].start()
    for c in nears:
        c.wait_recv()
    for c in local:
        c.wait()

    slab = wo.shape[0] // 4

    def o_rows(slot, quarter):
        return wo_s.at[slot, pl.ds(pl.multiple_of(quarter * slab, slab), slab), :]

    def o_half(i):
        return pl.ds(pl.multiple_of(quad * slab + i * (slab // 2), slab // 2), slab // 2)

    o_via = [remote(wo.at[o_half(i), :], wo_via.at[i], via_send.at[2 + i], via_recv.at[2 + i], {"sp": to}) for i, to in enumerate((right, left))]
    o_on = [remote(wo_via.at[i], wo_s.at[2, o_half(i), :], via_send.at[4 + i], via_recv.at[4 + i], {"sp": to}) for i, to in enumerate((right, left))]
    o_direct = [remote(wo.at[pl.ds(pl.multiple_of(quad * slab, slab), slab), :], o_rows(i, quad), o_send.at[i], o_recv.at[i], {"sp": to})
                for i, to in enumerate((right, left))]
    o_fars = [remote(o_rows(i, quad), o_rows(i, quad), o_far_send.at[i], o_far_recv.at[i], pal) for i in range(3)]
    o_nears = [[remote(o_rows(i, quarter), o_rows(i, quarter), o_near_send.at[m, i], o_near_recv.at[m, i], twin) for i in range(3)]
               for m, quarter in enumerate((quad, there))]

    def arrival(p, side):
        half = pl.ds(side * chunk, chunk)
        return remote(held.at[p, half, :], held.at[p, half, :], a_send.at[p - 2, side], a_recv.at[p - 2, side], {"sp": left if side else right})

    pieces = [(i, m) for i in range(kb) for m in range(g)]
    ones = jnp.ones((8, run), k_s.dtype)

    def reset():
        top_s[...] = jnp.full(top_s.shape, NEG, jnp.float32)
        mix_s[...] = jnp.zeros(mix_s.shape, jnp.float32)

    def block(block_q, j, masked):
        queries = pl.ds(pl.multiple_of(block_q * run, run), run)
        here = pl.ds(pl.multiple_of(j * run, run), run)
        if masked:
            ok = lax.broadcasted_iota(jnp.int32, (run, run), 1) >= lax.broadcasted_iota(jnp.int32, (run, run), 0)

        def score(i, m):
            return _dot(k_s[i, here, :], q_s[g * i + m, queries, :], 1, 1)

        scores = [score(*piece) for piece in pieces[:ahead]]
        for at, (i, m) in enumerate(pieces):
            if at + ahead < len(pieces):
                scores.append(score(*pieces[at + ahead]))
            s = jnp.where(ok, scores[at], HIDDEN) if masked else scores[at]
            own = slice(m * run, (m + 1) * run)
            old = top_s[i : i + 1, own]
            top = jnp.maximum(old, s.max(axis=0, keepdims=True))
            top_s[i : i + 1, own] = top
            p = jnp.exp2((s - top) * e).astype(k_s.dtype)
            values = jnp.concatenate([v_s[i, here, :].T, ones], axis=0)
            mix_s[i, :, own] = mix_s[i, :, own] * jnp.exp2((old - top) * e) + _dot(values, p, 1, 0)

    early_near, late_near = 3 - lax.rem(me, 2), 1 - lax.rem(me, 2)

    def pair(p, _):
        early, passed = p < 2, p >= 6
        firsts = (jnp.where(early, me * 4 + 2 * p, jnp.where(passed, over * 4 + p - 6, left * 4 + p - 2)),
                  jnp.where(early, me * 4 + 2 * p + 1, jnp.where(passed, over * 4 + 9 - p, right * 4 + 5 - p)))
        for side, at in enumerate(firsts):
            place = (lax.broadcasted_iota(jnp.int32, (chunk, HEAD), 0) + at * chunk).astype(jnp.float32)
            angle = place * freq_ref[...]
            cos_s[side * chunk : (side + 1) * chunk, :] = jnp.cos(angle)
            sign = jnp.where(lax.broadcasted_iota(jnp.int32, (chunk, HEAD), 1) < HEAD // 2, -1.0, 1.0)
            sin_s[side * chunk : (side + 1) * chunk, :] = sign * jnp.sin(angle)

        @pl.when(p == 6)
        def _():
            block_q = 2 * early_near + 1
            reset()
            lax.fori_loop(0, jnp.minimum(2 * over, block_q), lambda j, _: block(block_q, j, False), None)
            lax.fori_loop(2 * over + 2, block_q, lambda j, _: block(block_q, j, False), None)
            block(block_q, block_q, True)

        @pl.when(p >= 2)
        def _():
            for side in range(2):
                arrival(p, side).wait_recv()

        @pl.when((p >= 2) & (p < 4))
        def _():
            for side in range(2):
                half = pl.ds(side * chunk, chunk)
                remote(held.at[p, half, :], held.at[p + 4, half, :], a_send.at[p + 2, side], a_recv.at[p + 2, side], {"sp": left if side else right}).start()

        @pl.when(p == 6)
        def _():
            for c in (*o_via, *o_direct):
                c.start()

        for at in range(0, w.shape[1], wide):
            got = jnp.dot(held[p], w[:, at : at + wide], preferred_element_type=jnp.float32).astype(jnp.bfloat16)
            for h in range(at, at + wide, HEAD):
                t = got[:, h - at : h - at + HEAD]
                if h < nq + nk:
                    t = t.astype(jnp.float32)
                    t = (t * cos_s[...] + pltpu.roll(t, HEAD // 2, 1) * sin_s[...]).astype(jnp.bfloat16)
                for side, first in enumerate(firsts):
                    to = pl.ds(pl.multiple_of(first * chunk, chunk), chunk)
                    half = t[side * chunk : (side + 1) * chunk]
                    if h < nq:
                        q_s[h // HEAD, to, :] = half
                    elif h < nq + nk:
                        k_s[(h - nq) // HEAD, to, :] = half
                    else:
                        v_s[(h - nq - nk) // HEAD, to, :] = half

    lax.fori_loop(0, 8, pair, None)
    for c in (*direct, *passed_on, *fars, *nears):
        c.wait_send()
    for p in range(2, 8):
        for side in range(2):
            arrival(p, side).wait_send()
    for to in (right, left, over):
        pl.semaphore_signal(ready, inc=1, device_id={"sp": to}, device_id_type=pl.DeviceIdType.MESH)
    fill = [pltpu.make_async_copy(x.at[pl.ds(i * run, run), :], held.at[3 + i], x_sem.at[i]) for i in range(2)]
    fill += [pltpu.make_async_copy(wo.at[pl.ds(i * run, run), :], held.at[5 + i], own_sem.at[i]) for i in range(2)]
    for c in fill:
        c.start()

    def plan(i):
        owners = {"early": early_near, "over": over, "late": late_near, "own": me}
        owner, half = me, 1
        for at, (whose, which) in reversed(tuple(enumerate(ORDER))):
            owner, half = jnp.where(i == at, owners[whose], owner), jnp.where(i == at, which, half)
        return owner, half

    def seen_at(slot, t):
        row, col = lax.div(slot, 2) * rows + t * tile, lax.rem(slot, 2) * nq
        return w.at[pl.ds(pl.multiple_of(row, tile), tile), pl.ds(pl.multiple_of(col, nq), nq)]

    def staged(i):
        return held.at[lax.div(i, 2), :, pl.ds(pl.multiple_of(lax.rem(i, 2) * nq, nq), nq)]

    def back(i):
        owner, half = plan(i)
        rel = lax.rem(owner - me + n, n)
        slot = jnp.where(rel == 1, 0, jnp.where(rel == 3, 1, 2))
        copies = []
        for k in range(run // tile):
            t = half * (run // tile) + k
            frm = held.at[lax.div(i, 2), pl.ds(k * tile, tile), pl.ds(pl.multiple_of(lax.rem(i, 2) * nq, nq), nq)]
            copies.append(remote(frm, seen_at(slot, t), seen_send.at[slot, t], seen_recv.at[slot, t], {"sp": owner}))
        return copies

    def step(i, _):
        owner, half = plan(i)
        block_q = 2 * owner + half

        for when, these in ((3, (0, 1)), (5, (2,))):

            @pl.when(i == when)
            def _():
                for m in these:
                    for c in (o_on if m == 2 else o_direct[m : m + 1]):
                        c.wait_recv()
                    o_fars[m].start()
                    o_nears[0][m].start()

        @pl.when(i > 0)
        def _():
            reset()

        begin = jnp.where(i == 0, 2 * over, 0)
        end = jnp.where(i == 0, jnp.minimum(2 * over + 2, block_q), block_q)
        lax.fori_loop(begin, end, lambda j, _: block(block_q, j, False), None)

        @pl.when(i > 0)
        def _():
            block(block_q, block_q, True)

        def store(put):
            for i, m in pieces:
                o = mix_s[i, :HEAD, m * run : (m + 1) * run] * (1 / mix_s[i, HEAD : HEAD + 1, m * run : (m + 1) * run])
                put((g * i + m) * HEAD, o.T.astype(held.dtype))

        @pl.when(i == 0)
        def _():
            for m in range(2):
                o_via[m].wait_recv()
                o_on[m].start()
            pl.semaphore_wait(ready, 3)

        @pl.when(i < 6)
        def _():
            def put(at, o):
                staged(i)[:, at : at + HEAD] = o

            store(put)
            for c in back(i):
                c.start()

        @pl.when(i >= 6)
        def _():
            def put(at, o):
                w[pl.ds(pl.multiple_of(rows + half * run, run), run), nq + at : nq + at + HEAD] = o

            store(put)

    lax.fori_loop(0, 8, step, None)

    for m in range(3):
        o_fars[m].wait_recv()
        o_nears[1][m].start()
    for c in fill:
        c.wait()
    for m in range(2):
        for c in o_nears[m]:
            c.wait_recv()

    def done(t):
        per = run // tile
        at = pl.ds(pl.multiple_of(lax.rem(t, per) * tile, tile), tile)
        return pltpu.make_async_copy(held.at[3 + lax.div(t, per), at, :], y.at[pl.ds(pl.multiple_of(t * tile, tile), tile), :], out_sem.at[t])

    def finish(t, _):
        for m in range(3):
            remote(seen_at(m, t), seen_at(m, t), seen_send.at[m, t], seen_recv.at[m, t], {"sp": (left, right, over)[m]}).wait_recv()
        per = run // tile
        at, half = pl.ds(pl.multiple_of(lax.rem(t, per) * tile, tile), tile), lax.div(t, per)
        for c in range(0, d, wide):
            total = held[3 + half, at, c : c + wide].astype(jnp.float32)
            for m in range(4):
                tokens = pl.ds(pl.multiple_of(m // 2 * rows + t * tile, tile), tile)
                if m < 3:
                    total += jnp.dot(w[tokens, m % 2 * nq : (m % 2 + 1) * nq], wo_s[m, :, c : c + wide], preferred_element_type=jnp.float32)
                else:
                    for k in range(2):
                        total += jnp.dot(w[tokens, nq + k * run : nq + (k + 1) * run], held[5 + k, :, c : c + wide], preferred_element_type=jnp.float32)
            held[3 + half, at, c : c + wide] = total.astype(held.dtype)
        done(t).start()

    lax.fori_loop(0, rows // tile, finish, None)
    for t in range(rows // tile):
        done(t).wait()
    for i in range(6):
        for c in back(i):
            c.wait_send()
    for c in (*o_via, *o_on, *o_direct, *o_fars, *o_nears[0], *o_nears[1]):
        c.wait_send()


def layer(mesh, x, gain, wq, wk, wv, wo):
    n = mesh.shape["sp"]
    rows, d = x.shape
    tokens, heads, kb = rows * n, wq.shape[1] // (n * HEAD), wk.shape[1] // (n * HEAD)
    g, run = heads // kb, rows // 2
    freq = np.float32(THETA) ** (-np.arange(HEAD // 2, dtype=np.float32) / np.float32(HEAD // 2))
    freq = jnp.asarray(np.concatenate([freq, freq])[None])
    vmem = pl.BlockSpec(memory_space=pltpu.VMEM)
    bf, dma = jnp.bfloat16, pltpu.SemaphoreType.DMA
    return pl.pallas_call(
        functools.partial(_layer, n=n, scale=HEAD**-0.5, wide=512, ahead=3),
        in_specs=[ANY, vmem, vmem, ANY, ANY, ANY, ANY],
        out_specs=ANY,
        out_shape=jax.ShapeDtypeStruct((rows, d), bf),
        scratch_shapes=[
            pltpu.VMEM((8, run, d), bf), pltpu.VMEM((d, (heads + 2 * kb) * HEAD), bf), pltpu.VMEM((heads, tokens, HEAD), bf),
            pltpu.VMEM((kb, tokens, HEAD), bf), pltpu.VMEM((kb, tokens, HEAD), bf), pltpu.VMEM((3, *wo.shape), bf),
            pltpu.VMEM((run, HEAD), jnp.float32), pltpu.VMEM((run, HEAD), jnp.float32),
            pltpu.VMEM((kb, g * run), jnp.float32), pltpu.VMEM((kb, HEAD + 8, g * run), jnp.float32),
            pltpu.VMEM((2, wq.shape[0] // 8, d), bf), pltpu.VMEM((2, wo.shape[0] // 8, d), bf),
            dma((2,)), dma((3,)), dma((4, 3)), dma((4, 3)), dma((6,)), dma((6,)), dma((3,)), dma((3,)), dma((2, 3)), dma((2, 3)), dma((6, 2)), dma((6, 2)),
            dma((2,)), dma((2,)), dma((3,)), dma((3,)), dma((2, 3)), dma((2, 3)), dma((3, 4)), dma((3, 4)), dma((4,)), pltpu.SemaphoreType.REGULAR,
        ],
        compiler_params=pltpu.CompilerParams(collective_id=0, has_side_effects=True, vmem_limit_bytes=67043328),
        cost_estimate=pl.CostEstimate(flops=2 * heads * tokens * tokens * HEAD + 6 * tokens * d * heads * HEAD, transcendentals=heads * tokens * tokens // 2,
                                      bytes_accessed=2 * (2 * x.size + 4 * wo.size)),
        name="layer",
    )(x, gain[None], freq, wq, wk, wv, wo)


def solution(mesh):
    tokens, whole = P(("dp", "sp"), None), P("sp", None)
    return jax.shard_map(
        functools.partial(layer, mesh),
        mesh=mesh,
        in_specs=(tokens, P(None), whole, whole, whole, whole),
        out_specs=tokens,
        check_vma=False,
    )
```

```python
import functools

import jax
import jax.numpy as jnp
from jax import lax
from jax.experimental import pallas as pl
from jax.experimental.pallas import tpu as pltpu
import numpy as np
from jax.sharding import PartitionSpec as P

HEAD = 128
THETA = 10000
NEG = -1e30
HIDDEN = 2 * NEG
LOG2E = 1.4426950408889634
ANY = pl.BlockSpec(memory_space=pl.ANY)
ORDER = (("early", 1), ("late", 1), ("late", 0), ("early", 0), ("over", 0), ("over", 1), ("own", 0), ("own", 1))


def _dot(a, b, ca, cb):
    return lax.dot_general(a, b, (((ca,), (cb,)), ((), ())), preferred_element_type=jnp.float32)


def _layer(x, gain_ref, freq_ref, wq, wk, wv, wo, y, held, w, q_s, k_s, v_s, wo_s, cos_s, sin_s, top_s, mix_s, w_via, wo_via, x_sem, own_sem, w_send, w_recv,
           via_send, via_recv,
           w_far_send, w_far_recv, w_near_send, w_near_recv, a_send, a_recv, o_send, o_recv, o_far_send, o_far_recv, o_near_send, o_near_recv,
           seen_send, seen_recv, out_sem, ready, *, n, scale, wide, ahead):
    me, group = lax.axis_index("sp"), lax.axis_index("dp")
    right, left, over = lax.rem(me + 1, n), lax.rem(me + n - 1, n), lax.rem(me + 2, n)
    quad = lax.rem(group, 4)
    core, chip = lax.rem(quad, 2), lax.div(quad, 2)
    twin = {"dp": group + 1 - 2 * core}
    pal = {"dp": group + 2 - 4 * chip}
    there = quad + 2 - 4 * chip
    rows, d = x.shape
    run, chunk = rows // 2, rows // 4
    tile = 256
    heads, kb = q_s.shape[0], k_s.shape[0]
    g = heads // kb
    nq, nk = heads * HEAD, kb * HEAD
    e = scale * LOG2E

    fill = [pltpu.make_async_copy(x.at[pl.ds(i * run, run), :], held.at[i], x_sem.at[i]) for i in range(2)]
    for c in fill:
        c.start()
    barrier = pltpu.get_barrier_semaphore()
    for to in ({"sp": right}, {"sp": left}, {"sp": over}, twin, pal):
        pl.semaphore_signal(barrier, inc=1, device_id=to, device_id_type=pl.DeviceIdType.MESH)
    pl.semaphore_wait(barrier, 5)

    def remote(src, dst, send, recv, to):
        return pltpu.make_async_remote_copy(src_ref=src, dst_ref=dst, send_sem=send, recv_sem=recv, device_id=to, device_id_type=pl.DeviceIdType.MESH)

    depth = wq.shape[0]
    part = depth // 4
    kinds = ((wq, nq, 0), (wk, nk, nq), (wv, nk, nq + nk))
    direct = []
    for i, to in enumerate((right, left)):
        by = pl.ds(quad * part + i * (part // 2), part // 2)
        for j, (m, size, at) in enumerate(kinds):
            direct.append(remote(m.at[by, pl.ds(over * size, size)], w_via.at[i, :, pl.ds(at, size)], w_send.at[2 + i, j], w_recv.at[2 + i, j], {"sp": to}))
    for i, to in enumerate((right, left)):
        mine, there_at = pl.ds(quad * part, part), pl.ds(me * depth + quad * part, part)
        for j, (m, size, at) in enumerate(kinds):
            direct.append(remote(m.at[mine, pl.ds(to * size, size)], w.at[there_at, pl.ds(at, size)], w_send.at[i, j], w_recv.at[i, j], {"sp": to}))
    for c in direct:
        c.start()
    all_own = pl.ds(me * depth, depth)
    local = [pltpu.make_async_copy(m.at[:, pl.ds(me * size, size)], w.at[all_own, pl.ds(at, size)], own_sem.at[j])
             for j, (m, size, at) in enumerate(kinds)]
    for c in fill:
        c.wait()

    def norm(i, _):
        per = run // 128
        at = pl.ds(pl.multiple_of(lax.rem(i, per) * 128, 128), 128)
        wide_x = held[lax.div(i, per), at, :].astype(jnp.float32)
        rms = lax.rsqrt(jnp.mean(wide_x * wide_x, -1, keepdims=True) + 1e-6)
        held[lax.div(i, per), at, :] = (wide_x * rms * gain_ref[...].astype(jnp.float32)[None]).astype(jnp.bfloat16)

    lax.fori_loop(0, rows // 128, norm, None)
    for c in local:
        c.start()

    def states(c):
        return held.at[c // 2, pl.ds(c % 2 * chunk, chunk), :]

    upper, lower = pl.ds(0, chunk), pl.ds(chunk, chunk)
    sends = []
    for c in range(4):
        sends.append(remote(states(c), held.at[2 + c, upper, :], a_send.at[c, 0], a_recv.at[c, 0], {"sp": right}))
        sends.append(remote(states(3 - c), held.at[2 + c, lower, :], a_send.at[c, 1], a_recv.at[c, 1], {"sp": left}))
    for c in sends[:2]:
        c.start()
    passed_on = []
    for i, (frm, to) in enumerate(((left, right), (right, left))):
        for j in range(3):
            direct[3 * i + j].wait_recv()
        put = w.at[pl.ds(frm * depth + quad * part + i * (part // 2), part // 2), :]
        passed_on.append(remote(w_via.at[i], put, via_send.at[i], via_recv.at[i], {"sp": to}))
        passed_on[-1].start()
    for c in sends[2:]:
        c.start()

    def w_rows(frm, quarter):
        return w.at[pl.ds(frm * depth + quarter * part, part), :]

    sources = (left, right, over)
    fars, nears = [], []
    for i, frm in enumerate(sources):
        if i < 2:
            for j in range(3):
                direct[6 + 3 * i + j].wait_recv()
        else:
            for c in passed_on:
                c.wait_recv()
        fars.append(remote(w_rows(frm, quad), w_rows(frm, quad), w_far_send.at[i], w_far_recv.at[i], pal))
        nears.append(remote(w_rows(frm, quad), w_rows(frm, quad), w_near_send.at[0, i], w_near_recv.at[0, i], twin))
        fars[-1].start()
        nears[-1].start()
    for i, frm in enumerate(sources):
        fars[i].wait_recv()
        nears.append(remote(w_rows(frm, there), w_rows(frm, there), w_near_send.at[1, i], w_near_recv.at[1, i], twin))
        nears[-1].start()
    for c in nears:
        c.wait_recv()
    for c in local:
        c.wait()

    slab = wo.shape[0] // 4

    def o_rows(slot, quarter):
        return wo_s.at[slot, pl.ds(pl.multiple_of(quarter * slab, slab), slab), :]

    def o_half(i):
        return pl.ds(pl.multiple_of(quad * slab + i * (slab // 2), slab // 2), slab // 2)

    o_via = [remote(wo.at[o_half(i), :], wo_via.at[i], via_send.at[2 + i], via_recv.at[2 + i], {"sp": to}) for i, to in enumerate((right, left))]
    o_on = [remote(wo_via.at[i], wo_s.at[2, o_half(i), :], via_send.at[4 + i], via_recv.at[4 + i], {"sp": to}) for i, to in enumerate((right, left))]
    o_direct = [remote(wo.at[pl.ds(pl.multiple_of(quad * slab, slab), slab), :], o_rows(i, quad), o_send.at[i], o_recv.at[i], {"sp": to})
                for i, to in enumerate((right, left))]
    o_fars = [remote(o_rows(i, quad), o_rows(i, quad), o_far_send.at[i], o_far_recv.at[i], pal) for i in range(3)]
    o_nears = [[remote(o_rows(i, quarter), o_rows(i, quarter), o_near_send.at[m, i], o_near_recv.at[m, i], twin) for i in range(3)]
               for m, quarter in enumerate((quad, there))]

    def arrival(p, side):
        half = pl.ds(side * chunk, chunk)
        return remote(held.at[p, half, :], held.at[p, half, :], a_send.at[p - 2, side], a_recv.at[p - 2, side], {"sp": left if side else right})

    pieces = [(i, m) for i in range(kb) for m in range(g)]
    ones = jnp.ones((8, run), k_s.dtype)

    def reset():
        top_s[...] = jnp.full(top_s.shape, NEG, jnp.float32)
        mix_s[...] = jnp.zeros(mix_s.shape, jnp.float32)

    def block(block_q, j, masked):
        queries = pl.ds(pl.multiple_of(block_q * run, run), run)
        here = pl.ds(pl.multiple_of(j * run, run), run)
        if masked:
            ok = lax.broadcasted_iota(jnp.int32, (run, run), 1) >= lax.broadcasted_iota(jnp.int32, (run, run), 0)

        def score(i, m):
            return _dot(k_s[i, here, :], q_s[g * i + m, queries, :], 1, 1)

        scores = [score(*piece) for piece in pieces[:ahead]]
        for at, (i, m) in enumerate(pieces):
            if at + ahead < len(pieces):
                scores.append(score(*pieces[at + ahead]))
            s = jnp.where(ok, scores[at], HIDDEN) if masked else scores[at]
            own = slice(m * run, (m + 1) * run)
            old = top_s[i : i + 1, own]
            top = jnp.maximum(old, s.max(axis=0, keepdims=True))
            top_s[i : i + 1, own] = top
            p = jnp.exp2((s - top) * e).astype(k_s.dtype)
            values = jnp.concatenate([v_s[i, here, :].T, ones], axis=0)
            mix_s[i, :, own] = mix_s[i, :, own] * jnp.exp2((old - top) * e) + _dot(values, p, 1, 0)

    early_near, late_near = 3 - lax.rem(me, 2), 1 - lax.rem(me, 2)

    def pair(p, _):
        early, passed = p < 2, p >= 6
        firsts = (jnp.where(early, me * 4 + 2 * p, jnp.where(passed, over * 4 + p - 6, left * 4 + p - 2)),
                  jnp.where(early, me * 4 + 2 * p + 1, jnp.where(passed, over * 4 + 9 - p, right * 4 + 5 - p)))
        for side, at in enumerate(firsts):
            place = (lax.broadcasted_iota(jnp.int32, (chunk, HEAD), 0) + at * chunk).astype(jnp.float32)
            angle = place * freq_ref[...]
            cos_s[side * chunk : (side + 1) * chunk, :] = jnp.cos(angle)
            sign = jnp.where(lax.broadcasted_iota(jnp.int32, (chunk, HEAD), 1) < HEAD // 2, -1.0, 1.0)
            sin_s[side * chunk : (side + 1) * chunk, :] = sign * jnp.sin(angle)

        @pl.when(p == 6)
        def _():
            block_q = 2 * early_near + 1
            reset()
            lax.fori_loop(0, jnp.minimum(2 * over, block_q), lambda j, _: block(block_q, j, False), None)
            lax.fori_loop(2 * over + 2, block_q, lambda j, _: block(block_q, j, False), None)
            block(block_q, block_q, True)

        @pl.when(p >= 2)
        def _():
            for side in range(2):
                arrival(p, side).wait_recv()

        @pl.when((p >= 2) & (p < 4))
        def _():
            for side in range(2):
                half = pl.ds(side * chunk, chunk)
                remote(held.at[p, half, :], held.at[p + 4, half, :], a_send.at[p + 2, side], a_recv.at[p + 2, side], {"sp": left if side else right}).start()

        @pl.when(p == 6)
        def _():
            for c in (*o_via, *o_direct):
                c.start()

        for at in range(0, w.shape[1], wide):
            got = jnp.dot(held[p], w[:, at : at + wide], preferred_element_type=jnp.float32).astype(jnp.bfloat16)
            for h in range(at, at + wide, HEAD):
                t = got[:, h - at : h - at + HEAD]
                if h < nq + nk:
                    t = t.astype(jnp.float32)
                    t = (t * cos_s[...] + pltpu.roll(t, HEAD // 2, 1) * sin_s[...]).astype(jnp.bfloat16)
                for side, first in enumerate(firsts):
                    to = pl.ds(pl.multiple_of(first * chunk, chunk), chunk)
                    half = t[side * chunk : (side + 1) * chunk]
                    if h < nq:
                        q_s[h // HEAD, to, :] = half
                    elif h < nq + nk:
                        k_s[(h - nq) // HEAD, to, :] = half
                    else:
                        v_s[(h - nq - nk) // HEAD, to, :] = half

    lax.fori_loop(0, 8, pair, None)
    for c in (*direct, *passed_on, *fars, *nears):
        c.wait_send()
    for p in range(2, 8):
        for side in range(2):
            arrival(p, side).wait_send()
    for to in (right, left, over):
        pl.semaphore_signal(ready, inc=1, device_id={"sp": to}, device_id_type=pl.DeviceIdType.MESH)
    fill = [pltpu.make_async_copy(x.at[pl.ds(i * run, run), :], held.at[3 + i], x_sem.at[i]) for i in range(2)]
    fill += [pltpu.make_async_copy(wo.at[pl.ds(i * run, run), :], held.at[5 + i], own_sem.at[i]) for i in range(2)]
    for c in fill:
        c.start()

    def plan(i):
        owners = {"early": early_near, "over": over, "late": late_near, "own": me}
        owner, half = me, 1
        for at, (whose, which) in reversed(tuple(enumerate(ORDER))):
            owner, half = jnp.where(i == at, owners[whose], owner), jnp.where(i == at, which, half)
        return owner, half

    def seen_at(slot, t):
        row, col = lax.div(slot, 2) * rows + t * tile, lax.rem(slot, 2) * nq
        return w.at[pl.ds(pl.multiple_of(row, tile), tile), pl.ds(pl.multiple_of(col, nq), nq)]

    def staged(i):
        return held.at[lax.div(i, 2), :, pl.ds(pl.multiple_of(lax.rem(i, 2) * nq, nq), nq)]

    def back(i):
        owner, half = plan(i)
        rel = lax.rem(owner - me + n, n)
        slot = jnp.where(rel == 1, 0, jnp.where(rel == 3, 1, 2))
        copies = []
        for k in range(run // tile):
            t = half * (run // tile) + k
            frm = held.at[lax.div(i, 2), pl.ds(k * tile, tile), pl.ds(pl.multiple_of(lax.rem(i, 2) * nq, nq), nq)]
            copies.append(remote(frm, seen_at(slot, t), seen_send.at[slot, t], seen_recv.at[slot, t], {"sp": owner}))
        return copies

    def step(i, _):
        owner, half = plan(i)
        block_q = 2 * owner + half

        for when, these in ((3, (0, 1)), (5, (2,))):

            @pl.when(i == when)
            def _():
                for m in these:
                    for c in (o_on if m == 2 else o_direct[m : m + 1]):
                        c.wait_recv()
                    o_fars[m].start()
                    o_nears[0][m].start()

        @pl.when(i > 0)
        def _():
            reset()

        begin = jnp.where(i == 0, 2 * over, 0)
        end = jnp.where(i == 0, jnp.minimum(2 * over + 2, block_q), block_q)
        lax.fori_loop(begin, end, lambda j, _: block(block_q, j, False), None)

        @pl.when(i > 0)
        def _():
            block(block_q, block_q, True)

        def store(put):
            for i, m in pieces:
                o = mix_s[i, :HEAD, m * run : (m + 1) * run] * (1 / mix_s[i, HEAD : HEAD + 1, m * run : (m + 1) * run])
                put((g * i + m) * HEAD, o.T.astype(held.dtype))

        @pl.when(i == 0)
        def _():
            for m in range(2):
                o_via[m].wait_recv()
                o_on[m].start()
            pl.semaphore_wait(ready, 3)

        @pl.when(i < 6)
        def _():
            def put(at, o):
                staged(i)[:, at : at + HEAD] = o

            store(put)
            for c in back(i):
                c.start()

        @pl.when(i >= 6)
        def _():
            def put(at, o):
                w[pl.ds(pl.multiple_of(rows + half * run, run), run), nq + at : nq + at + HEAD] = o

            store(put)

    lax.fori_loop(0, 8, step, None)

    for m in range(3):
        o_fars[m].wait_recv()
        o_nears[1][m].start()
    for c in fill:
        c.wait()
    for m in range(2):
        for c in o_nears[m]:
            c.wait_recv()

    def done(t):
        per = run // tile
        at = pl.ds(pl.multiple_of(lax.rem(t, per) * tile, tile), tile)
        return pltpu.make_async_copy(held.at[3 + lax.div(t, per), at, :], y.at[pl.ds(pl.multiple_of(t * tile, tile), tile), :], out_sem.at[t])

    def finish(t, _):
        for m in range(3):
            remote(seen_at(m, t), seen_at(m, t), seen_send.at[m, t], seen_recv.at[m, t], {"sp": (left, right, over)[m]}).wait_recv()
        per = run // tile
        at, half = pl.ds(pl.multiple_of(lax.rem(t, per) * tile, tile), tile), lax.div(t, per)
        for c in range(0, d, wide):
            total = held[3 + half, at, c : c + wide].astype(jnp.float32)
            for m in range(4):
                tokens = pl.ds(pl.multiple_of(m // 2 * rows + t * tile, tile), tile)
                if m < 3:
                    total += jnp.dot(w[tokens, m % 2 * nq : (m % 2 + 1) * nq], wo_s[m, :, c : c + wide], preferred_element_type=jnp.float32)
                else:
                    for k in range(2):
                        total += jnp.dot(w[tokens, nq + k * run : nq + (k + 1) * run], held[5 + k, :, c : c + wide], preferred_element_type=jnp.float32)
            held[3 + half, at, c : c + wide] = total.astype(held.dtype)
        done(t).start()

    lax.fori_loop(0, rows // tile, finish, None)
    for t in range(rows // tile):
        done(t).wait()
    for i in range(6):
        for c in back(i):
            c.wait_send()
    for c in (*o_via, *o_on, *o_direct, *o_fars, *o_nears[0], *o_nears[1]):
        c.wait_send()


def layer(mesh, x, gain, wq, wk, wv, wo):
    n = mesh.shape["sp"]
    rows, d = x.shape
    tokens, heads, kb = rows * n, wq.shape[1] // (n * HEAD), wk.shape[1] // (n * HEAD)
    g, run = heads // kb, rows // 2
    freq = np.float32(THETA) ** (-np.arange(HEAD // 2, dtype=np.float32) / np.float32(HEAD // 2))
    freq = jnp.asarray(np.concatenate([freq, freq])[None])
    vmem = pl.BlockSpec(memory_space=pltpu.VMEM)
    bf, dma = jnp.bfloat16, pltpu.SemaphoreType.DMA
    return pl.pallas_call(
        functools.partial(_layer, n=n, scale=HEAD**-0.5, wide=512, ahead=3),
        in_specs=[ANY, vmem, vmem, ANY, ANY, ANY, ANY],
        out_specs=ANY,
        out_shape=jax.ShapeDtypeStruct((rows, d), bf),
        scratch_shapes=[
            pltpu.VMEM((8, run, d), bf), pltpu.VMEM((d, (heads + 2 * kb) * HEAD), bf), pltpu.VMEM((heads, tokens, HEAD), bf),
            pltpu.VMEM((kb, tokens, HEAD), bf), pltpu.VMEM((kb, tokens, HEAD), bf), pltpu.VMEM((3, *wo.shape), bf),
            pltpu.VMEM((run, HEAD), jnp.float32), pltpu.VMEM((run, HEAD), jnp.float32),
            pltpu.VMEM((kb, g * run), jnp.float32), pltpu.VMEM((kb, HEAD + 8, g * run), jnp.float32),
            pltpu.VMEM((2, wq.shape[0] // 8, d), bf), pltpu.VMEM((2, wo.shape[0] // 8, d), bf),
            dma((2,)), dma((3,)), dma((4, 3)), dma((4, 3)), dma((6,)), dma((6,)), dma((3,)), dma((3,)), dma((2, 3)), dma((2, 3)), dma((6, 2)), dma((6, 2)),
            dma((2,)), dma((2,)), dma((3,)), dma((3,)), dma((2, 3)), dma((2, 3)), dma((3, 4)), dma((3, 4)), dma((4,)), pltpu.SemaphoreType.REGULAR,
        ],
        compiler_params=pltpu.CompilerParams(collective_id=0, has_side_effects=True, vmem_limit_bytes=67043328),
        cost_estimate=pl.CostEstimate(flops=2 * heads * tokens * tokens * HEAD + 6 * tokens * d * heads * HEAD, transcendentals=heads * tokens * tokens // 2,
                                      bytes_accessed=2 * (2 * x.size + 4 * wo.size)),
        name="layer",
    )(x, gain, freq, wq, wk, wv, wo)


def solution(mesh):
    tokens, whole = P(("dp", "sp"), None), P("sp", None)
    return jax.shard_map(
        functools.partial(layer, mesh),
        mesh=mesh,
        in_specs=(tokens, P(None), whole, whole, whole, whole),
        out_specs=tokens,
        check_vma=False,
    )
```
